32 devices in a mesh: gx: 8 (over z, y), row: 2 (over x), ta: 2 (over core).
Axes of the slice: x: 2, y: 2, z: 4, core: 2. Of those that a mesh axis runs over, the one named last changes fastest.
Arguments:
- conserved: float32 [5, 64, 64, 256], P(None, 'gx', 'row', 'ta'), may hold values from -6 to 6
- diffusivity: float32 [5], replicated, may hold values from 0.02 to 0.1
- axial_speed: float32 [5], replicated, may hold values from 0.2 to 0.6
- coupling: float32 [5, 5], replicated, may hold values from -0.6 to 0.6
- pressure_weights: float32 [5], replicated, may hold values from 0.5 to 1.5
- station_cell: int32 [512], P(('gx', 'row')), may hold values from 0 to 4095, as said below
- owner_row: int32 [512, 1], P(('gx', 'row')), may hold values from 0 to 1; in each aligned block of 32 rows (0 to 31, 32 to 63, ...) at most 16 rows name the same one
- window_table: int32 [4], replicated, may hold values from 1 to 8
Outputs:
- advanced: float32 [5, 64, 64, 256], P(None, 'gx', 'row', 'ta')
- spectra: float32 [16, 32, 1056], P(('gx', 'row'), 'ta')
The draws below stay inside these ranges and needn't reach their ends.
Inputs may be any that keep to these rules, and one draw needn't show every extreme that they name: `station_cell`: entries b * 32 to (b + 1) * 32 - 1, with b = g * 2 + j, are distinct cells whose axial index lies in [g * 8, (g + 1) * 8) and radial index in [j * 32, (j + 1) * 32). `owner_row`: in each aligned block of 32 stations, no owner is named more than 16 times.
All inputs are finite; a program needn't handle non-finite values.
Results may differ from the reference program's by a relative error of at most 0.00013.
Values sent between devices are 32-bit elements; how exact they have to be, the bound alone decides.
No kernel may reach another device: no remote copies, remote signals or barrier semaphores. Data moves between devices by JAX's collectives and lax.ppermute only.
A program may use at most 64 MiB of HBM per device.

```python
import math
import jax
import jax.numpy as jnp
import numpy as np
from jax import lax

CX = 8
CR = 32
NTH = 256
NM = 33
NFREQ = 16
STEPS = 4
STN_DEV = 32
CAP = 16
NX = 64
NR = 64
STATIONS = 512
N_GX = 8
N_ROW = 2


def draw_station_cell(key, part):
    tiles = N_GX * N_ROW
    block_keys = jax.random.split(jax.random.fold_in(key, 11), tiles)
    chosen = jax.vmap(lambda single: jax.random.permutation(single, CX * CR)[:STN_DEV])(block_keys)
    block_index = jnp.arange(tiles, dtype=jnp.int32)
    cell_x = (block_index // N_ROW)[:, None] * CX + chosen // CR
    cell_r = (block_index % N_ROW)[:, None] * CR + chosen % CR
    return (cell_x * NR + cell_r).reshape(-1).astype(jnp.int32)


def set_ends(result, stream_key, low, top_value):
    longest = result.shape.index(max(result.shape))
    spots = []
    for shift in (0, 1):
        where = [jax.random.randint(jax.random.fold_in(stream_key, axis), (), 0, length) for axis, length in enumerate(result.shape)]
        where[longest] = (where[longest] + shift) % result.shape[longest]
        spots.append(tuple(where))
    return result.at[spots[0]].set(low).at[spots[1]].set(top_value)


def level_of(key, extent, shards, low, largest):
    factor_of = 1.0
    for dim, blocks in shards:
        draws = jax.random.uniform(jax.random.fold_in(jax.random.fold_in(key, 6), dim), (blocks,), jnp.float32, low / len(shards), largest / len(shards))
        factor_of = factor_of * jnp.repeat(jnp.exp(draws), extent[dim] // blocks).reshape((-1,) + (1,) * (len(extent) - 1 - dim))
    return factor_of


def deal_out(rng, own, number, rows, amount, top, reach, skew):
    sequence = jax.random.permutation(rng, amount)
    crowded, common = portions_of(amount, rows * top, reach, skew, True), portions_of(amount, rows * top, reach, skew, False)
    places = jnp.arange(amount)

    def named(sizes, rotation):
        used = int((sizes > 0).sum())
        fixed = max(1, used // 4)
        moved = fixed + (places - fixed + rotation * (used - fixed)) % max(1, amount - fixed)
        return jnp.zeros((amount,), jnp.int32).at[sequence[jnp.where(places < fixed, places, moved)]].set(jnp.asarray(sizes, jnp.int32))

    sizes = jnp.where(number % 4 == 0, named(crowded, number // 4), named(common, number - number // 4 - 1))
    mixed = jax.random.permutation(jax.random.fold_in(own, 3), amount)
    giver, sink = mixed[0:amount // 2 * 2:2], mixed[1:amount // 2 * 2:2]
    room = jnp.minimum(sizes[giver] - 1, reach - sizes[sink]) // 2
    room = jnp.where((giver == sequence[0]) | (sink == sequence[0]) | (sizes[sink] == 0), 0, jnp.maximum(room, 0))
    moved = jax.random.randint(jax.random.fold_in(own, 4), (amount // 2,), 0, 1 << 20) % (room + 1)
    sizes = sizes.at[giver].add(-moved).at[sink].add(moved)
    items = jnp.searchsorted(jnp.cumsum(sizes), jnp.arange(rows * top), side="right").astype(jnp.int32)
    listing = items.reshape(top, rows).T
    listing = listing[jax.random.permutation(jax.random.fold_in(own, 1), rows)]
    rotation = jax.random.randint(jax.random.fold_in(own, 2), (rows, 1), 0, top)
    return jnp.take_along_axis(listing, (jnp.arange(top)[None, :] + rotation) % top, axis=1)


def portions_of(number_of, total, limit, slope, full):
    portions = [(1 << 20) // math.isqrt(grade ** slope) + 1 for grade in range(1, number_of + 1)]
    largest = limit if full else min(limit, max(-(-total // number_of), total * portions[0] // sum(portions)))
    least = 1 if total - largest >= number_of - 1 else 0
    counts, spare = [largest] + [least] * (number_of - 1), total - largest - least * (number_of - 1)
    while spare > 0:
        movable = [i for i in range(1, number_of) if counts[i] < largest] or [i for i in range(1, number_of) if counts[i] < limit]
        mass, left = sum([portions[i] for i in movable]), spare
        for i in movable:
            extra = min(limit - counts[i], max(1, left * portions[i] // mass), spare)
            counts[i] = counts[i] + extra
            spare = spare - extra
    return np.array(counts)


def centred(stream_key, dims, deviation, bound, pieces=(), kind=jnp.bfloat16):
    drawn = jax.random.normal(stream_key, dims, jnp.float32) * deviation
    if len(pieces) > 0:
        drawn = level_of(stream_key, dims, pieces, -0.22, 0.18) * drawn
    return jnp.clip(drawn, min=-bound, max=bound).astype(kind)


def setup_inputs(seed: int = 0) -> dict:
    keys = jax.random.split(jax.random.key(seed), 9)
    conserved = centred(keys[0], (5, NX, NR, NTH), 1.0, 6.0, ((1, 8), (2, 2), (3, 2)), jnp.float32)
    diffusivity = jnp.clip(jnp.exp(jax.random.uniform(keys[1], (5,), jnp.float32, math.log(0.02), math.log(0.1))), 0.02, 0.1)
    axial_speed = jnp.clip(jax.random.uniform(keys[2], (5,), jnp.float32, 0.2, 0.6), 0.2, 0.6)
    coupling = centred(keys[3], (5, 5), 0.15, 0.6, (), jnp.float32)
    pressure_weights = jnp.clip(jax.random.uniform(keys[4], (5,), jnp.float32, 0.5, 1.5), 0.5, 1.5)
    station_cell = draw_station_cell(jax.random.fold_in(keys[8], 71), 0)
    owner_row_keys = jax.random.split(jax.random.fold_in(keys[6], 1), STATIONS // STN_DEV)
    owner_row_turns = jax.random.permutation(jax.random.fold_in(keys[6], 3), STATIONS // STN_DEV)
    owner_row = jax.vmap(lambda own, number: deal_out(jax.random.fold_in(keys[6], 2), own, number, STN_DEV, N_ROW, 1, CAP, 2))(owner_row_keys, owner_row_turns).reshape((STATIONS, 1))
    window_table = set_ends(jax.random.randint(keys[7], (STEPS,), 1, 9), jax.random.fold_in(keys[7], 1), 1, 8).astype(jnp.int32)
    return dict(conserved=conserved, diffusivity=diffusivity, axial_speed=axial_speed, coupling=coupling, pressure_weights=pressure_weights, station_cell=station_cell, owner_row=owner_row, window_table=window_table)


exact_mode = lax.Precision.HIGHEST

def change_of(padded, rate, velocity):
    lengths = (padded.shape[0] - 4, padded.shape[1] - 4, padded.shape[2] - 4)

    def shifted(offset_x, offset_r, offset_t):
        return padded[offset_x:offset_x + lengths[0], offset_r:offset_r + lengths[1], offset_t:offset_t + lengths[2]]
    center = shifted(2, 2, 2)
    near = shifted(3, 2, 2) + shifted(1, 2, 2) + shifted(2, 3, 2) + shifted(2, 1, 2) + shifted(2, 2, 3) + shifted(2, 2, 1)
    far = shifted(4, 2, 2) + shifted(0, 2, 2) + shifted(2, 4, 2) + shifted(2, 0, 2) + shifted(2, 2, 4) + shifted(2, 2, 0)
    laplace = (16.0 * near - far - 90.0 * center) / 12.0
    gradient = (8.0 * (shifted(3, 2, 2) - shifted(1, 2, 2)) - (shifted(4, 2, 2) - shifted(0, 2, 2))) / 12.0
    return rate * laplace - velocity * gradient

def azimuth_table(offset, count, total, modes):
    theta = offset + jnp.arange(count, dtype=jnp.int32)
    order = jnp.arange(modes, dtype=jnp.int32)
    turns = theta[:, None] * order[None, :] % total
    angle = 2.0 * math.pi / total * turns.astype(jnp.float32)
    return jnp.concatenate([jnp.cos(angle), jnp.sin(angle)], axis=1) * (1.0 / math.sqrt(total))

def spectral_increment(coeffs, weight, step_index, modes, freqs):
    cosine_part = coeffs[..., :modes]
    sine_part = coeffs[..., modes:]
    phase = math.pi * step_index / freqs * jnp.arange(1, freqs + 1, dtype=jnp.float32)
    cos_phase = jnp.cos(phase)[:, None]
    sin_phase = jnp.sin(phase)[:, None]
    real_part = cos_phase * cosine_part[..., None, :] - sin_phase * sine_part[..., None, :]
    imag_part = -(sin_phase * cosine_part[..., None, :] + cos_phase * sine_part[..., None, :])
    return weight * jnp.stack([real_part, imag_part], axis=-2)

def reference(conserved, diffusivity, axial_speed, coupling, pressure_weights, station_cell, owner_row, window_table):
    state = conserved
    pos_x = station_cell // NR
    pos_r = station_cell % NR
    table = azimuth_table(0, NTH, NTH, NM)
    totals = jnp.zeros((STATIONS, NFREQ, 2, NM), jnp.float32)
    for step_index in range(STEPS):
        padded = jnp.pad(state, ((0, 0), (2, 2), (2, 2), (0, 0)))
        padded = jnp.concatenate([padded[..., -2:], padded, padded[..., :2]], axis=3)
        change = lax.map(lambda item: change_of(item[0], item[1], item[2]), (padded, diffusivity, axial_speed))
        mixed = jnp.einsum('fg,gxrt->fxrt', coupling, state, precision=exact_mode)
        state = state + change + mixed
        pressure = jnp.einsum('f,fxrt->xrt', pressure_weights, state, precision=exact_mode)
        cycles = pressure[pos_x, pos_r]
        coeffs = jnp.dot(cycles, table, precision=exact_mode)
        weight = window_table[step_index].astype(jnp.float32) / 8.0
        totals = totals + spectral_increment(coeffs, weight, step_index, NM, NFREQ)
    owners = owner_row[:, 0].reshape(-1, STN_DEV)
    ordinal = jnp.arange(STN_DEV, dtype=jnp.int32)
    earlier = ordinal[None, :] < ordinal[:, None]
    same_owner = owners[:, None, :] == owners[:, :, None]
    rank = lax.optimization_barrier(jnp.sum((earlier[None] & same_owner).astype(jnp.int32), axis=2))
    block_index = jnp.arange(owners.shape[0], dtype=jnp.int32)
    row_out = (block_index // N_ROW * N_ROW)[:, None] + owners
    column = (block_index % N_ROW * CAP)[:, None] + rank
    spectra = jnp.zeros((N_GX * N_ROW, N_ROW * CAP, NFREQ * 2 * NM), jnp.float32)
    spectra = spectra.at[row_out.reshape(-1), column.reshape(-1)].add(totals.reshape(STATIONS, NFREQ * 2 * NM))
    return (state, spectra)
```

```python
import functools
import math

import jax
import jax.numpy as jnp
import numpy as np
from jax import lax
from jax.experimental import pallas as pl
from jax.experimental.pallas import tpu as pltpu
from jax.sharding import PartitionSpec as P

NM = 33
NFREQ = 16
STEPS = 4
CAP = 16
HALO = 2 * STEPS
NCOEF = 11
PAD = 8

VMEM = pltpu.VMEM
SMEM = pltpu.SMEM


def mode_basis(total, cores):
    theta = np.arange(total)
    wave = []
    for m in range(NM):
        wave.append((m, 0))
    wave.append((total // 2, 0))
    for m in range(1, NM):
        wave.append((m, 1))
    for m in range(NM, total // 2):
        wave.append((m, 0))
        wave.append((m, 1))
    rows, turns = [], []
    for m, kind in wave:
        angle = 2.0 * math.pi * ((m * theta) % total) / total
        row = np.sin(angle) if kind else np.cos(angle)
        norm = 1.0 / total if m in (0, total // 2) else 2.0 / total
        rows.append(row * math.sqrt(norm))
        turns.append(2.0 * math.pi * m / total)
    basis = np.stack(rows).reshape(cores, total // cores, total)
    turns = np.array(turns)
    eigen = (32.0 * np.cos(turns) - 2.0 * np.cos(2.0 * turns) - 30.0) / 12.0
    return basis, eigen.reshape(cores, total // cores)


def split_const(table):
    table = np.asarray(table, np.float32)
    high = table.astype(jnp.bfloat16)
    low = (table - high.astype(np.float32)).astype(jnp.bfloat16)
    return high, low


def spectrum_table(lanes):
    out = np.zeros((STEPS, lanes, NFREQ, 2, NM))
    for t in range(STEPS):
        phase = math.pi * t / NFREQ * np.arange(1, NFREQ + 1)
        for m in range(NM):
            scale = 1.0 if m == 0 else math.sqrt(0.5)
            out[t, m, :, 0, m] = np.cos(phase) * scale
            out[t, m, :, 1, m] = -np.sin(phase) * scale
            if m > 0:
                out[t, NM + m, :, 0, m] = -np.sin(phase) * scale
                out[t, NM + m, :, 1, m] = -np.cos(phase) * scale
    return out.reshape(STEPS, lanes, NFREQ * 2 * NM)


def halves(x):
    high = x.astype(jnp.bfloat16)
    return high, (x - high.astype(jnp.float32)).astype(jnp.bfloat16)


def dot3(high, low, table_high, table_low):
    dot = functools.partial(jnp.dot, preferred_element_type=jnp.float32)
    return dot(high, table_high) + (dot(low, table_high) + dot(high, table_low))


def forward_kernel(peers, sizes, *refs):
    pieces = refs[: sizes["ta"]]
    hi_ref, lo_ref, va_ref, vb_ref, e0_ref, ep_ref, ec_ref = refs[sizes["ta"] :]
    fields, cx, cr, ct = pieces[0].shape
    core = lax.axis_index("ta")
    row = lax.axis_index("row")
    odd = lax.axis_index("gx") % 2
    table_high, table_low = hi_ref[core], lo_ref[core]
    half = cx // 2
    keep = HALO - 2
    pair_at, cross_at = (cx - keep) * (1 - odd), (cx - keep) * odd
    for f in range(fields):
        x = jnp.concatenate([p[f].reshape(cx * cr, ct) for p in pieces], axis=1)
        high, low = halves(x)
        v = dot3(high, low, table_high, table_low).reshape(cx, cr, ct)
        va_ref[:, f] = v[:half]
        vb_ref[:, f] = v[half:]
        if peers == 2:
            edges = [jnp.where(row == 0, v[:, cr - HALO :], v[:, :HALO])]
        else:
            edges = [v[:, cr - HALO :], v[:, :HALO]]
        for side, edge in enumerate(edges):
            e0_ref[side, :, f] = edge
    for side in range(e0_ref.shape[0]):
        ep_ref[side] = e0_ref[side, pl.ds(pair_at, keep)]
        ec_ref[side] = e0_ref[side, pl.ds(cross_at, keep)]


def update_kernel(
    peers, sizes, coef_ref, weight_ref, index_ref,
    va_ref, vb_ref, p1a_ref, p1b_ref, p2a_ref, p2b_ref, r0_ref, rp_ref, rc_ref,
    out_ref, cycle_ref, w0_ref, w1_ref,
):
    half, fields, cr, lanes = va_ref.shape
    cx = 2 * half
    keep = HALO - 2
    gx, row, core = lax.axis_index("gx"), lax.axis_index("row"), lax.axis_index("ta")
    odd = gx % 2
    rows = w0_ref.shape[2] - 2 * PAD
    blocks = rows // 8
    if peers == 2:
        own = pl.multiple_of(PAD + HALO * row, 8)
        spots = [pl.multiple_of(PAD + cr * (1 - row), 8)]
    else:
        own = PAD + HALO
        spots = [PAD, PAD + HALO + cr]
    left_open = (gx > 0).astype(jnp.int32)
    right_open = (gx < sizes["gx"] - 1).astype(jnp.int32)
    pair_at = 2 * cx * (1 - odd)
    cross_at = 2 * cx * odd
    zero = jnp.zeros((8, lanes), jnp.float32)

    def clear(x, carry):
        for f in range(fields):
            for w in (w0_ref, w1_ref):
                w[x, f, pl.ds(0, PAD)] = zero
                w[x, f, pl.ds(PAD + rows, PAD)] = zero
        return carry

    lax.fori_loop(0, 3 * cx, clear, 0)

    def place(src_ref, at, r):
        n = src_ref.shape[0]
        h = src_ref.shape[2]

        def one(i, carry):
            for f in range(fields):
                w0_ref[at + i, f, pl.ds(r, h)] = src_ref[i, f]
            return carry

        lax.fori_loop(0, n, one, 0)

    place(va_ref, cx, own)
    place(vb_ref, cx + half, own)
    place(p1a_ref, pair_at, own)
    place(p1b_ref, pair_at + half, own)
    place(p2a_ref, cross_at, own)
    place(p2b_ref, cross_at + half, own)
    for side, spot in enumerate(spots):
        place(r0_ref.at[side], cx, spot)
        place(rp_ref.at[side], pair_at + (cx - keep) * odd, spot)
        place(rc_ref.at[side], cross_at + (cx - keep) * (1 - odd), spot)

    def blank(x, carry):
        for f in range(fields):
            for b in range(blocks):
                w1_ref[x, f, pl.ds(PAD + 8 * b, 8)] = zero
        return carry

    lax.fori_loop(cx - 2, cx - 2 + 2 * (1 - left_open), blank, 0)
    lax.fori_loop(2 * cx, 2 * cx + 2 * (1 - right_open), blank, 0)

    def layer(src, store, x, base, count):
        v = [
            [src[x, f, pl.ds(base + 8 * b, 8)] for b in range(count)]
            for f in range(fields)
        ]
        for f in range(fields):
            c = [coef_ref[f, i] for i in range(NCOEF)]
            for b in range(count):
                r = base + 8 * b
                total = c[0] * v[0][b]
                for g in range(1, fields):
                    total = total + c[g] * v[g][b]
                near = src[x, f, pl.ds(r + 1, 8)] + src[x, f, pl.ds(r - 1, 8)]
                far = src[x, f, pl.ds(r + 2, 8)] + src[x, f, pl.ds(r - 2, 8)]
                side = c[fields] * near + c[fields + 1] * far
                one = c[fields + 2] * src[x + 1, f, pl.ds(r, 8)] + c[fields + 3] * src[x - 1, f, pl.ds(r, 8)]
                two = c[fields + 4] * src[x + 2, f, pl.ds(r, 8)] + c[fields + 5] * src[x - 2, f, pl.ds(r, 8)]
                store(x, f, b, (total + side) + (one + two))

    def gather(t, read):
        @pl.when(core == 0)
        def _():
            def station(s, carry):
                x, r, slot = index_ref[0, s], index_ref[1, s], index_ref[2, s]
                p = weight_ref[0] * read(x, 0, r)
                for f in range(1, fields):
                    p = p + weight_ref[f] * read(x, f, r)
                cycle_ref[t, pl.ds(slot, 1)] = p
                return carry

            lax.fori_loop(0, index_ref.shape[1], station, 0, unroll=8)

    cycle_ref[...] = jnp.zeros_like(cycle_ref)
    buffers = [w0_ref, w1_ref]
    for t in range(STEPS):
        src, dst = buffers[t % 2], buffers[(t + 1) % 2]
        reach = HALO - 2 * (t + 1)
        low = cx - reach * left_open
        high = 2 * cx + reach * right_open
        if t < STEPS - 1:

            def store(x, f, b, value, dst=dst):
                dst[x, f, pl.ds(PAD + 8 * b, 8)] = value

            def body(x, carry, src=src, store=store):
                layer(src, store, x, PAD, blocks)
                return carry

            lax.fori_loop(low, high, body, 0)
            if peers > 2:
                for edge, spot in ((0, spots[0]), (peers - 1, spots[1])):

                    @pl.when(row == edge)
                    def _(spot=spot, dst=dst, low=low, high=high):
                        def wipe(x, carry):
                            for f in range(fields):
                                dst[x, f, pl.ds(spot, HALO)] = jnp.zeros((HALO, lanes), jnp.float32)
                            return carry

                        lax.fori_loop(low, high, wipe, 0)

            gather(t, lambda x, f, r, dst=dst: dst[cx + x, f, pl.ds(own + r, 1)])
        else:

            def store_out(x, f, b, value):
                out_ref[x - cx, f, pl.ds(8 * b, 8)] = value

            def body_out(x, carry, src=src):
                layer(src, store_out, x, own, cr // 8)
                return carry

            lax.fori_loop(cx, 2 * cx, body_out, 0)
            gather(t, lambda x, f, r: out_ref[x, f, pl.ds(r, 1)])


def inverse_kernel(cores, *refs):
    pieces = refs[:cores]
    hi_ref, lo_ref, out_ref = refs[cores:]
    fields, cx, cr, ct = out_ref.shape
    core = lax.axis_index("ta")
    table_high, table_low = hi_ref[core], lo_ref[core]
    for f in range(fields):
        x = jnp.concatenate([p[:, f].reshape(cx * cr, ct) for p in pieces], axis=1)
        high, low = halves(x)
        out_ref[f] = dot3(high, low, table_high, table_low).reshape(cx, cr, ct)


def spectra_kernel(peers, cores, *refs):
    received = refs[:peers]
    window_ref, hi_ref, lo_ref, out_ref = refs[peers:]
    share = peers // cores
    first = lax.axis_index("ta") * share
    mine = lax.axis_index("row")
    rows = []
    for j in range(share):
        hop = (mine - (first + j) + peers) % peers
        value = jnp.where(hop == 0, received[0][...], 0.0)
        for k in range(1, peers):
            value = value + jnp.where(hop == k, received[k][...], 0.0)
        rows.append(value)
    x = rows[0] if share == 1 else jnp.concatenate(rows, axis=1)
    total = None
    for t in range(STEPS):
        weight = window_ref[t].astype(jnp.float32) * 0.125
        high, low = halves(x[t] * weight)
        part = dot3(high, low, hi_ref[t], lo_ref[t])
        total = part if total is None else total + part
    out_ref[0] = total


def spec(space, n):
    return [pl.BlockSpec(memory_space=space)] * n


def local(
    sizes,
    conserved,
    diffusivity,
    axial_speed,
    coupling,
    pressure_weights,
    station_cell,
    owner_row,
    window_table,
):
    fields, cx, cr, ct = conserved.shape
    nx, peers, cores = sizes["gx"], sizes["row"], sizes["ta"]
    assert cx == HALO and nx % 2 == 0 and peers % cores == 0
    total_r, total_t = cr * peers, ct * cores
    gx, row, core = lax.axis_index("gx"), lax.axis_index("row"), lax.axis_index("ta")
    half, keep = cx // 2, HALO - 2
    sides = 1 if peers == 2 else 2
    basis, eigen = mode_basis(total_t, cores)
    ahead = np.zeros((cores, total_t, ct))
    back = np.zeros((cores, total_t, ct))
    for c in range(cores):
        for k in range(cores):
            d = (c + k) % cores
            here = slice(k * ct, (k + 1) * ct)
            ahead[c, here] = basis[c][:, d * ct : (d + 1) * ct].T
            back[c, here] = basis[d][:, c * ct : (c + 1) * ct]

    def around(x):
        return [x] + [
            lax.ppermute(x, "ta", [((c + k) % cores, c) for c in range(cores)])
            for k in range(1, cores)
        ]

    tile = jax.ShapeDtypeStruct((half, fields, cr, ct), jnp.float32)
    edge = jax.ShapeDtypeStruct((sides, cx, fields, HALO, ct), jnp.float32)
    corner = jax.ShapeDtypeStruct((sides, keep, fields, HALO, ct), jnp.float32)
    va, vb, e0, ep, ec = pl.pallas_call(
        functools.partial(forward_kernel, peers, sizes),
        out_shape=(tile, tile, edge, corner, corner),
        in_specs=spec(VMEM, cores + 2),
        out_specs=tuple(spec(VMEM, 5)),
        name="forward",
    )(*around(conserved), *split_const(ahead))

    swap = [(i, i ^ 1) for i in range(nx)]
    forward = [(i, i + 2 if i % 2 == 0 else i - 2) for i in range(nx)]
    forward = [(a, b) for a, b in forward if 0 <= b < nx]
    cross = [(i, i - 1 if i % 2 == 0 else i + 1) for i in range(nx)]
    cross = [(a, b) for a, b in cross if 0 <= b < nx]
    p1a = lax.ppermute(va, "gx", swap)
    p1b = lax.ppermute(vb, "gx", swap)

    def radial(x, hops):
        got = []
        for side in range(sides):
            if peers == 2:
                turn = [(0, 1), (1, 0)]
            else:
                turn = [(r, r + 1) for r in range(peers - 1)]
                if side:
                    turn = [(b, a) for a, b in turn]
            pairs = [(a * peers + c, b * peers + d) for a, b in hops for c, d in turn]
            got.append(lax.ppermute(x[side : side + 1], ("gx", "row"), pairs))
        return got[0] if sides == 1 else jnp.concatenate(got, axis=0)

    r0 = radial(e0, [(i, i) for i in range(nx)])
    rp = radial(ep, swap)
    rc = radial(ec, cross)
    p2a = lax.ppermute(p1a, "gx", forward)
    p2b = lax.ppermute(p1b, "gx", forward)

    eigenvalue = jnp.asarray(eigen, jnp.float32)[core]
    rate, speed = diffusivity, axial_speed
    middle = 1.0 + rate[:, None] * (eigenvalue[None, :] - 5.0)
    mix = coupling[:, :, None] + jnp.eye(fields, dtype=jnp.float32)[:, :, None] * middle[:, None, :]
    line = jnp.stack(
        [
            rate * (16.0 / 12.0),
            rate * (-1.0 / 12.0),
            (16.0 * rate - 8.0 * speed) / 12.0,
            (16.0 * rate + 8.0 * speed) / 12.0,
            (speed - rate) / 12.0,
            -(speed + rate) / 12.0,
        ],
        axis=1,
    )
    coef = jnp.concatenate([mix, jnp.broadcast_to(line[:, :, None], (fields, 6, ct))], axis=1)
    coef = jnp.broadcast_to(coef[:, :, None, :], (fields, NCOEF, 8, ct))

    owners = owner_row[:, 0]
    ordinal = jnp.arange(owners.shape[0], dtype=jnp.int32)
    earlier = (ordinal[None, :] < ordinal[:, None]) & (owners[None, :] == owners[:, None])
    rank = jnp.sum(earlier.astype(jnp.int32), axis=1)
    index = jnp.stack(
        [
            station_cell // total_r - gx * cx,
            station_cell % total_r - row * cr,
            owners * CAP + rank,
        ]
    )

    rows = cr + HALO * sides + 2 * PAD
    work = pltpu.VMEM((3 * cx, fields, rows, ct), jnp.float32)
    modes, cycles = pl.pallas_call(
        functools.partial(update_kernel, peers, sizes),
        out_shape=(
            jax.ShapeDtypeStruct((cx, fields, cr, ct), jnp.float32),
            jax.ShapeDtypeStruct((STEPS, peers * CAP, ct), jnp.float32),
        ),
        in_specs=spec(VMEM, 1) + spec(SMEM, 2) + spec(VMEM, 9),
        out_specs=tuple(spec(VMEM, 2)),
        scratch_shapes=[work, work],
        name="update",
    )(coef, pressure_weights, index, va, vb, p1a, p1b, p2a, p2b, r0, rp, rc)

    share = peers // cores
    received = []
    for k in range(peers):
        pairs = []
        for j in range(peers):
            pairs.append((j * cores, (j + k) % peers * cores + j // share))
        start = (row + k) % peers * CAP
        block = lax.dynamic_slice_in_dim(cycles, start, CAP, axis=1)
        received.append(lax.ppermute(block, ("row", "ta"), pairs))

    advanced = pl.pallas_call(
        functools.partial(inverse_kernel, cores),
        out_shape=jax.ShapeDtypeStruct(conserved.shape, jnp.float32),
        in_specs=spec(VMEM, cores + 2),
        out_specs=pl.BlockSpec(memory_space=VMEM),
        name="inverse",
    )(*around(modes), *split_const(back))
    spectra = pl.pallas_call(
        functools.partial(spectra_kernel, peers, cores),
        out_shape=jax.ShapeDtypeStruct((1, share * CAP, NFREQ * 2 * NM), jnp.float32),
        in_specs=spec(VMEM, peers) + spec(SMEM, 1) + spec(VMEM, 2),
        out_specs=pl.BlockSpec(memory_space=VMEM),
        name="spectra",
    )(*received, window_table, *split_const(spectrum_table(ct)))
    return (advanced, spectra)


def solution(mesh):
    in_specs = (
        P(None, "gx", "row", "ta"),
        P(),
        P(),
        P(),
        P(),
        P(("gx", "row")),
        P(("gx", "row"), None),
        P(),
    )
    out_specs = (P(None, "gx", "row", "ta"), P(("gx", "row"), "ta", None))
    body = functools.partial(local, dict(mesh.shape))
    return jax.shard_map(body, mesh=mesh, in_specs=in_specs, out_specs=out_specs, check_vma=False)
```

```python
import functools
import math

import jax
import jax.numpy as jnp
import numpy as np
from jax import lax
from jax.experimental import pallas as pl
from jax.experimental.pallas import tpu as pltpu
from jax.sharding import PartitionSpec as P


NM = 33
NFREQ = 16
STEPS = 4
CAP = 16
HALO = 2 * STEPS
NCOEF = 11
PAD = 8
PIECES = 4
STRIP = 4

VMEM = pltpu.VMEM
SMEM = pltpu.SMEM
HBM = pltpu.HBM


def mode_basis(total, cores):
    theta = np.arange(total)
    wave = []
    for m in range(NM):
        wave.append((m, 0))
    wave.append((total // 2, 0))
    for m in range(1, NM):
        wave.append((m, 1))
    for m in range(NM, total // 2):
        wave.append((m, 0))
        wave.append((m, 1))
    rows, turns = [], []
    for m, kind in wave:
        angle = 2.0 * math.pi * ((m * theta) % total) / total
        row = np.sin(angle) if kind else np.cos(angle)
        norm = 1.0 / total if m in (0, total // 2) else 2.0 / total
        rows.append(row * math.sqrt(norm))
        turns.append(2.0 * math.pi * m / total)
    basis = np.stack(rows).reshape(cores, total // cores, total)
    turns = np.array(turns)
    eigen = (32.0 * np.cos(turns) - 2.0 * np.cos(2.0 * turns) - 30.0) / 12.0
    return basis, eigen.reshape(cores, total // cores)


def split_const(table):
    table = np.asarray(table, np.float32)
    high = table.astype(jnp.bfloat16)
    low = (table - high.astype(np.float32)).astype(jnp.bfloat16)
    return np.stack([high, low])


def spectrum_table(lanes):
    out = np.zeros((STEPS, lanes, NFREQ, 2, NM))
    for t in range(STEPS):
        phase = math.pi * t / NFREQ * np.arange(1, NFREQ + 1)
        for m in range(NM):
            scale = 1.0 if m == 0 else math.sqrt(0.5)
            out[t, m, :, 0, m] = np.cos(phase) * scale
            out[t, m, :, 1, m] = -np.sin(phase) * scale
            if m > 0:
                out[t, NM + m, :, 0, m] = -np.sin(phase) * scale
                out[t, NM + m, :, 1, m] = -np.cos(phase) * scale
    return out.reshape(STEPS, lanes, NFREQ * 2 * NM)


def halves(x):
    high = x.astype(jnp.bfloat16)
    return high, (x - high.astype(jnp.float32)).astype(jnp.bfloat16)


def dot3(high, low, table_high, table_low):
    dot = functools.partial(jnp.dot, preferred_element_type=jnp.float32)
    return dot(high, table_high) + (dot(low, table_high) + dot(high, table_low))


def position(sizes):
    gx, row, core = lax.axis_index("gx"), lax.axis_index("row"), lax.axis_index("ta")
    share = sizes["row"] // sizes["ta"]
    return gx, row, core, (core - row // share + sizes["ta"]) % sizes["ta"]


def stage_kernel(sizes, own_ref, table_ref, part_ref):
    fields, cx, cr, ct = own_ref.shape
    _, _, core, group = position(sizes)
    for f in range(fields):
        x = own_ref[f].reshape(cx * cr, ct)
        v = dot3(*halves(x), table_ref[0, group, core], table_ref[1, group, core])
        part_ref[:, f] = v.reshape(cx, cr, ct)


def forward_kernel(sizes, first, count, last, part_ref, table_ref, *refs):
    peers, cores = sizes["row"], sizes["ta"]
    sources, refs = refs[: cores - 1], refs[cores - 1 :]
    fields, cx, cr, ct = sources[0].shape
    _, row, core, group = position(sizes)
    step = cx // PIECES
    done = ()
    if last:
        done, refs = refs[:first], refs[first:]
    out = refs[:count]
    for f in range(fields):
        v = part_ref[first * step : (first + count) * step, f].reshape(count * step * cr, ct)
        for k, s in enumerate(sources):
            x = s[f, first * step : (first + count) * step].reshape(count * step * cr, ct)
            other = (core + k + 1) % cores
            v = v + dot3(*halves(x), table_ref[0, group, other], table_ref[1, group, other])
        v = v.reshape(count, step, cr, ct)
        for i in range(count):
            out[i][:, f] = v[i]
    if last:
        (e0_ref,) = refs[count:]
        for i, ref in enumerate(tuple(done) + tuple(out)):
            for side in range(e0_ref.shape[0]):
                top = 1 - row if peers == 2 else 1 - side
                rows = pl.ds(pl.multiple_of((cr - HALO) * top, 8), HALO)
                e0_ref[side, i * step : (i + 1) * step] = ref[:, :, rows]


def prepare_kernel(
    sizes, cx, cr, rate_ref, speed_ref, mix_ref, cell_ref, owner_ref, eigen_ref,
    coef_ref, place_ref, slots_ref, count_ref,
):
    peers = sizes["row"]
    fields = coef_ref.shape[0]
    shape = coef_ref.shape[2:]
    gx, row, _, group = position(sizes)
    eigen = eigen_ref[group]
    for f in range(fields):
        rate, speed = rate_ref[f], speed_ref[f]
        for g in range(fields):
            value = jnp.full(shape, mix_ref[f, g])
            if g == f:
                value = value + (1.0 + rate * (eigen - 5.0))
            coef_ref[f, g] = value
        line = [
            rate * (16.0 / 12.0),
            rate * (-1.0 / 12.0),
            (16.0 * rate - 8.0 * speed) * (1.0 / 12.0),
            (16.0 * rate + 8.0 * speed) * (1.0 / 12.0),
            (speed - rate) * (1.0 / 12.0),
            (speed + rate) * (-1.0 / 12.0),
        ]
        for i, value in enumerate(line):
            coef_ref[f, fields + i] = jnp.full(shape, value)
    slots_ref[...] = jnp.zeros_like(slots_ref)
    for o in range(peers):
        count_ref[o] = 0
    cells = lax.broadcasted_iota(jnp.int32, (1, cx * cr), 1)

    def station(s, carry):
        owner, cell = owner_ref[s], cell_ref[s]
        rank = count_ref[owner]
        count_ref[owner] = rank + 1
        slot = (owner - row + peers) % peers * CAP + rank
        here = (cell // (cr * peers) - gx * cx) * cr + cell % (cr * peers) - row * cr
        slots_ref[pl.ds(slot, 1)] = (cells == here).astype(jnp.float32)
        return carry

    lax.fori_loop(0, cell_ref.shape[0], station, 0)
    place_ref[...] = slots_ref[...].astype(jnp.bfloat16)


class Frame:
    def __init__(self, sizes, cx, cr, work_ref):
        self.peers, self.cx, self.cr = sizes["row"], cx, cr
        self.fields, self.lanes = work_ref.shape[1], work_ref.shape[3]
        self.rows = work_ref.shape[2] - 2 * PAD
        self.blocks = self.rows // 8
        gx, self.row, self.core, self.group = position(sizes)
        self.odd = gx % 2
        self.even = 1 - self.odd
        self.left = (gx > 0).astype(jnp.int32)
        self.right = (gx < sizes["gx"] - 1).astype(jnp.int32)
        self.sides = 1 if self.peers == 2 else 2
        self.own = PAD + HALO * self.row if self.peers == 2 else PAD + HALO
        if self.peers == 2:
            self.own = pl.multiple_of(self.own, 8)
        self.pair_at = 2 * cx * self.even
        self.far_at = 2 * cx * self.odd

    def halo(self, side):
        if self.peers == 2:
            return PAD + self.cr * (1 - self.row)
        return self.own - HALO if side == 0 else self.own + self.cr

    def clear(self, low, high, *works):
        zero = jnp.zeros((PAD, self.lanes), jnp.float32)

        def one(x, carry):
            for f in range(self.fields):
                for w in works:
                    w[x, f, pl.ds(0, PAD)] = zero
                    w[x, f, pl.ds(PAD + self.rows, PAD)] = zero
            return carry

        lax.fori_loop(low, high, one, 0)

    def blank(self, low, high, work):
        zero = jnp.zeros((8, self.lanes), jnp.float32)

        def one(x, carry):
            for f in range(self.fields):
                for b in range(self.blocks):
                    work[x, f, pl.ds(PAD + 8 * b, 8)] = zero
            return carry

        lax.fori_loop(low, high, one, 0)

    def place(self, source, work, at, r, low=0, high=None):
        h = source.shape[2]

        def one(i, carry):
            for f in range(self.fields):
                work[at + i, f, pl.ds(r, h)] = source[i, f]
            return carry

        lax.fori_loop(low, source.shape[0] if high is None else high, one, 0)

    def place_edge(self, edge_ref, work, at):
        for side in range(self.sides):
            self.place(edge_ref.at[side], work, at, pl.multiple_of(self.halo(side), 8))

    def layer(self, coef_ref, src, store, x, base, count):
        fields = self.fields
        v = [[src[x, f, pl.ds(base + 8 * b, 8)] for b in range(count)] for f in range(fields)]
        for f in range(fields):
            c = [coef_ref[f, i] for i in range(NCOEF)]
            for b in range(count):
                r = base + 8 * b
                total = c[0] * v[0][b]
                for g in range(1, fields):
                    total = total + c[g] * v[g][b]
                near = src[x, f, pl.ds(r + 1, 8)] + src[x, f, pl.ds(r - 1, 8)]
                far = src[x, f, pl.ds(r + 2, 8)] + src[x, f, pl.ds(r - 2, 8)]
                side = c[fields] * near + c[fields + 1] * far
                one = c[fields + 2] * src[x + 1, f, pl.ds(r, 8)] + c[fields + 3] * src[x - 1, f, pl.ds(r, 8)]
                two = c[fields + 4] * src[x + 2, f, pl.ds(r, 8)] + c[fields + 5] * src[x - 2, f, pl.ds(r, 8)]
                store(x, f, b, (total + side) + (one + two))

    def sweep(self, coef_ref, src, dst, low, high):
        def store(x, f, b, value):
            dst[x, f, pl.ds(PAD + 8 * b, 8)] = value

        def body(x, carry):
            self.layer(coef_ref, src, store, x, PAD, self.blocks)
            return carry

        lax.fori_loop(low, high, body, 0)
        if self.peers > 2:
            for side, edge in ((0, 0), (1, self.peers - 1)):

                @pl.when(self.row == edge)
                def _(side=side):
                    def wipe(x, carry):
                        for f in range(self.fields):
                            dst[x, f, pl.ds(self.halo(side), HALO)] = jnp.zeros(
                                (HALO, self.lanes), jnp.float32
                            )
                        return carry

                    lax.fori_loop(low, high, wipe, 0)

    def pressure(self, weight_ref, p_ref, t, read, low, high):
        def one(x, carry):
            for b in range(self.cr // 8):
                p = weight_ref[0] * read(x, 0, 8 * b)
                for f in range(1, self.fields):
                    p = p + weight_ref[f] * read(x, f, 8 * b)
                p_ref[t, pl.ds(pl.multiple_of((x - self.cx) * self.cr + 8 * b, 8), 8)] = p
            return carry

        lax.fori_loop(low, high, one, 0)


def near_kernel(sizes, coef_ref, weight_ref, *refs):
    own_refs, pair_refs = refs[:PIECES], refs[PIECES : 2 * PIECES]
    r0_ref, rp_ref, strip_ref, p_ref, w0_ref, w1_ref = refs[2 * PIECES :]
    step, cr = own_refs[0].shape[0], own_refs[0].shape[2]
    cx = step * PIECES
    z = Frame(sizes, cx, cr, w0_ref)
    first = cx * z.even
    z.clear(first, first + 2 * cx, w0_ref, w1_ref)
    for i in range(PIECES):
        z.place(own_refs[i], w0_ref, cx + i * step, z.own)
        z.place(pair_refs[i], w0_ref, z.pair_at + i * step, z.own)
    z.place_edge(r0_ref, w0_ref, cx)
    z.place_edge(rp_ref, w0_ref, z.pair_at)
    p_ref[...] = jnp.zeros_like(p_ref)
    works = [w0_ref, w1_ref]
    for t in range(1, STEPS):
        src, dst = works[(t - 1) % 2], works[t % 2]
        low = (cx + 2 * t) * z.even + 2 * t * z.odd
        high = (3 * cx - 2 * t) * z.even + (2 * cx - 2 * t) * z.odd
        z.sweep(coef_ref, src, dst, low, high)
        edge = low * z.even + (high - STRIP) * z.odd
        for i in range(STRIP):
            strip_ref[t - 1, i] = dst[edge + i, :, pl.ds(PAD, z.rows)]
        z.pressure(
            weight_ref, p_ref, t - 1,
            lambda x, f, r, dst=dst: dst[x, f, pl.ds(z.own + r, 8)],
            cx + 2 * t * z.even, 2 * cx - 2 * t * z.odd,
        )


def far_kernel(sizes, coef_ref, weight_ref, place_ref, *refs):
    own_refs, far_refs = refs[:PIECES], refs[PIECES : 2 * PIECES]
    r0_ref, rc_ref, strip_ref, part_ref, out_ref = refs[2 * PIECES : 2 * PIECES + 5]
    cycle_refs = refs[2 * PIECES + 5 : -3]
    w0_ref, w1_ref, p_ref = refs[-3:]
    step, cr = own_refs[0].shape[0], own_refs[0].shape[2]
    cx = step * PIECES
    z = Frame(sizes, cx, cr, w0_ref)
    first = cx * z.odd
    z.clear(first, first + 2 * cx, w0_ref, w1_ref)
    for i in range(PIECES):
        z.place(own_refs[i], w0_ref, cx + i * step, z.own)
        z.place(far_refs[i], w0_ref, z.far_at + i * step, z.own)
    z.place_edge(r0_ref, w0_ref, cx)
    z.place_edge(rc_ref, w0_ref, z.far_at)
    z.blank(cx - 2, cx - 2 + 2 * (1 - z.left), w1_ref)
    z.blank(2 * cx, 2 * cx + 2 * (1 - z.right), w1_ref)
    works = [w0_ref, w1_ref]
    for t in range(1, STEPS):
        src, dst = works[(t - 1) % 2], works[t % 2]
        reach = HALO - 2 * t
        low = (cx - reach * z.left) * z.even + (2 * cx - 2 * t) * z.odd
        high = (cx + 2 * t) * z.even + (2 * cx + reach * z.right) * z.odd
        z.sweep(coef_ref, src, dst, low, high)
        edge = (cx + 2 * t) * z.even + (2 * cx - 2 * t - STRIP) * z.odd
        for i in range(STRIP):
            dst[edge + i, :, pl.ds(PAD, z.rows)] = strip_ref[t - 1, i]
        p_ref[t - 1] = part_ref[t - 1]
        z.pressure(
            weight_ref, p_ref, t - 1,
            lambda x, f, r, dst=dst: dst[x, f, pl.ds(z.own + r, 8)],
            cx * z.even + (2 * cx - 2 * t) * z.odd, (cx + 2 * t) * z.even + 2 * cx * z.odd,
        )
    src = works[(STEPS - 1) % 2]

    def store_out(x, f, b, value):
        out_ref[x - cx, f, pl.ds(8 * b, 8)] = value

    def body_out(x, carry):
        z.layer(coef_ref, src, store_out, x, z.own, cr // 8)
        return carry

    lax.fori_loop(cx, 2 * cx, body_out, 0)
    z.pressure(weight_ref, p_ref, STEPS - 1, lambda x, f, r: out_ref[x - cx, f, pl.ds(r, 8)], cx, 2 * cx)
    dot = functools.partial(jnp.dot, preferred_element_type=jnp.float32)
    for t in range(STEPS):
        high, low = halves(p_ref[t])
        picked = dot(place_ref[...], high) + dot(place_ref[...], low)
        for k, ref in enumerate(cycle_refs):
            ref[t] = picked[k * CAP : (k + 1) * CAP]


def inverse_kernel(sizes, *refs):
    cores = sizes["ta"]
    sources = refs[:cores]
    table_ref, out_ref, x_ref, sems = refs[cores:]
    fields, cx, cr, ct = out_ref.shape
    _, _, core, group = position(sizes)
    table = [
        jnp.concatenate([table_ref[i, (group + k) % cores, core] for k in range(cores)], axis=0)
        for i in range(2)
    ]
    copies = []
    for f in range(fields):
        x = jnp.concatenate([s[:, f].reshape(cx * cr, ct) for s in sources], axis=1)
        x_ref[f] = dot3(*halves(x), *table).reshape(cx, cr, ct)
        copies.append(pltpu.make_async_copy(x_ref.at[f], out_ref.at[f], sems.at[f]))
        copies[f].start()
    for copy in copies:
        copy.wait()


def spectra_kernel(sizes, *refs):
    peers = sizes["row"]
    received = refs[:peers]
    window_ref, table_ref, out_ref = refs[peers:]
    _, row, core, _ = position(sizes)
    share = peers // sizes["ta"]
    blocks = []
    for j in range(share):
        hop = (row - (core * share + j) + peers) % peers
        value = jnp.where(hop == 0, received[0][...], 0.0)
        for k in range(1, peers):
            value = jnp.where(hop == k, received[k][...], value)
        blocks.append(value)
    x = blocks[0] if share == 1 else jnp.concatenate(blocks, axis=1)
    n = x.shape[1]
    dot = functools.partial(jnp.dot, preferred_element_type=jnp.float32)
    total = None
    for t in range(0, STEPS, 2):
        pair = jnp.concatenate(
            [x[i] * (window_ref[i].astype(jnp.float32) * 0.125) for i in (t, t + 1)], axis=1
        )
        high, low = halves(pair)
        both = dot(jnp.concatenate([high, low], axis=0), table_ref[0, t // 2])
        part = both[:n] + both[n:] + dot(high, table_ref[1, t // 2])
        total = part if total is None else total + part
    out_ref[0] = total


def spec(space, n):
    return [pl.BlockSpec(memory_space=space)] * n


def limit(mib):
    return pltpu.CompilerParams(vmem_limit_bytes=mib << 20)


def work_for(flops):
    return pl.CostEstimate(flops=flops, bytes_accessed=10**6, transcendentals=0)


def local(
    sizes,
    conserved,
    diffusivity,
    axial_speed,
    coupling,
    pressure_weights,
    station_cell,
    owner_row,
    window_table,
):
    fields, cx, cr, ct = conserved.shape
    nx, peers, cores = sizes["gx"], sizes["row"], sizes["ta"]
    assert cx == HALO and nx % 2 == 0 and peers % cores == 0
    share = peers // cores
    step = cx // PIECES
    sides = 1 if peers == 2 else 2
    basis, eigen = mode_basis(ct * cores, cores)
    blocks = basis.reshape(cores, ct, cores, ct).transpose(0, 2, 3, 1)
    ahead = split_const(blocks)
    back = split_const(blocks.transpose(0, 1, 3, 2))

    def shape(*dims):
        return jax.ShapeDtypeStruct(dims, jnp.float32)

    def others(x):
        return [
            lax.ppermute(x, "ta", [((c + k) % cores, c) for c in range(cores)])
            for k in range(1, cores)
        ]

    sources = others(conserved)
    part = pl.pallas_call(
        functools.partial(stage_kernel, sizes),
        out_shape=shape(cx, fields, cr, ct),
        in_specs=spec(VMEM, 2),
        out_specs=pl.BlockSpec(memory_space=VMEM),
        compiler_params=limit(8),
        cost_estimate=work_for(10**7),
        name="stage",
    )(conserved, ahead)
    tile = shape(step, fields, cr, ct)
    edge = shape(sides, cx, fields, HALO, ct)
    early = PIECES // 2
    own = list(
        pl.pallas_call(
            functools.partial(forward_kernel, sizes, 0, early, False),
            out_shape=(tile,) * early,
            in_specs=spec(VMEM, cores + 1),
            out_specs=tuple(spec(VMEM, early)),
            compiler_params=limit(8),
            cost_estimate=work_for(10**6),
            name="forward_early",
        )(part, ahead, *sources)
    )
    *rest, e0 = pl.pallas_call(
        functools.partial(forward_kernel, sizes, early, PIECES - early, True),
        out_shape=(tile,) * (PIECES - early) + (edge,),
        in_specs=spec(VMEM, cores + 1 + early),
        out_specs=tuple(spec(VMEM, PIECES - early + 1)),
        compiler_params=limit(8),
        cost_estimate=work_for(10**6),
        name="forward_late",
    )(part, ahead, *sources, *own)
    own += rest

    swap = [(i, i ^ 1) for i in range(nx)]
    onward = [(i, i + 2 if i % 2 == 0 else i - 2) for i in range(nx)]
    onward = [(a, b) for a, b in onward if 0 <= b < nx]

    r0 = []
    for side in range(sides):
        if peers == 2:
            turn = [(0, 1), (1, 0)]
        else:
            turn = [(r, r + 1) for r in range(peers - 1)]
            if side:
                turn = [(b, a) for a, b in turn]
        hops = [
            (r * cores + (g + r // share) % cores, q * cores + (g + q // share) % cores)
            for r, q in turn
            for g in range(cores)
        ]
        r0.append(lax.ppermute(e0[side : side + 1], ("row", "ta"), hops))
    r0 = r0[0] if sides == 1 else jnp.concatenate(r0, axis=0)
    pair, far = [], []
    for x in own:
        pair.append(lax.ppermute(x, "gx", swap))
    rp = lax.ppermute(r0, "gx", swap)
    rc = lax.ppermute(rp, "gx", onward)
    for x in pair:
        far.append(lax.ppermute(x, "gx", onward))

    lines = np.broadcast_to(eigen[:, None, :], (cores, 8, ct)).astype(np.float32)
    coef, place = pl.pallas_call(
        functools.partial(prepare_kernel, sizes, cx, cr),
        out_shape=(
            shape(fields, NCOEF, 8, ct),
            jax.ShapeDtypeStruct((peers * CAP, cx * cr), jnp.bfloat16),
        ),
        in_specs=spec(SMEM, 5) + spec(VMEM, 1),
        out_specs=tuple(spec(VMEM, 2)),
        scratch_shapes=[
            pltpu.VMEM((peers * CAP, cx * cr), jnp.float32),
            pltpu.SMEM((peers,), jnp.int32),
        ],
        compiler_params=limit(4),
        cost_estimate=work_for(10**6),
        name="prepare",
    )(diffusivity, axial_speed, coupling, station_cell, owner_row.reshape(-1), lines)

    rows = cr + HALO * sides
    work = pltpu.VMEM((3 * cx, fields, rows + 2 * PAD, ct), jnp.float32)
    strip, parts = pl.pallas_call(
        functools.partial(near_kernel, sizes),
        out_shape=(shape(STEPS - 1, STRIP, fields, rows, ct), shape(STEPS - 1, cx * cr, ct)),
        in_specs=spec(VMEM, 1) + spec(SMEM, 1) + spec(VMEM, 2 * PIECES + 2),
        out_specs=tuple(spec(VMEM, 2)),
        scratch_shapes=[work, work],
        compiler_params=limit(20),
        cost_estimate=work_for(10**7),
        name="near",
    )(coef, pressure_weights, *own, *pair, r0, rp)
    modes, *cycles = pl.pallas_call(
        functools.partial(far_kernel, sizes),
        out_shape=(shape(cx, fields, cr, ct),) + (shape(STEPS, CAP, ct),) * peers,
        in_specs=spec(VMEM, 1) + spec(SMEM, 1) + spec(VMEM, 1 + 2 * PIECES + 4),
        out_specs=tuple(spec(VMEM, 1 + peers)),
        scratch_shapes=[work, work, pltpu.VMEM((STEPS, cx * cr, ct), jnp.float32)],
        compiler_params=limit(20),
        cost_estimate=work_for(10**7),
        name="rest",
    )(coef, pressure_weights, place, *own, *far, r0, rc, strip, parts)

    received = [cycles[0]]
    for k in range(1, peers):
        pairs = []
        for j in range(peers):
            pairs.append((j * cores + j // share, (j + k) % peers * cores + j // share))
        received.append(lax.ppermute(cycles[k], ("row", "ta"), pairs))

    advanced = pl.pallas_call(
        functools.partial(inverse_kernel, sizes),
        out_shape=jax.ShapeDtypeStruct(conserved.shape, jnp.float32),
        in_specs=spec(VMEM, cores + 1),
        out_specs=pl.BlockSpec(memory_space=HBM),
        scratch_shapes=[pltpu.VMEM(conserved.shape, jnp.float32), pltpu.SemaphoreType.DMA((fields,))],
        compiler_params=limit(8),
        cost_estimate=work_for(10**6),
        name="inverse",
    )(modes, *others(modes), back)
    spectra = pl.pallas_call(
        functools.partial(spectra_kernel, sizes),
        out_shape=shape(1, share * CAP, NFREQ * 2 * NM),
        in_specs=spec(VMEM, peers) + spec(SMEM, 1) + spec(VMEM, 1),
        out_specs=pl.BlockSpec(memory_space=VMEM),
        compiler_params=limit(8),
        cost_estimate=work_for(10**6),
        name="spectra",
    )(*received, window_table, split_const(spectrum_table(ct).reshape(STEPS // 2, 2 * ct, -1)))
    return (advanced, spectra)


def solution(mesh):
    in_specs = (
        P(None, "gx", "row", "ta"),
        P(),
        P(),
        P(),
        P(),
        P(("gx", "row")),
        P(("gx", "row"), None),
        P(),
    )
    out_specs = (P(None, "gx", "row", "ta"), P(("gx", "row"), "ta", None))

    def body(*args):
        return local(dict(mesh.shape), *args)

    return jax.shard_map(body, mesh=mesh, in_specs=in_specs, out_specs=out_specs, check_vma=False)
```

```python
import functools
import math

import jax
import jax.numpy as jnp
import numpy as np
from jax import lax
from jax.experimental import pallas as pl
from jax.experimental.pallas import tpu as pltpu
from jax.sharding import PartitionSpec as P


NM = 33
NFREQ = 16
STEPS = 4
CAP = 16
HALO = 2 * STEPS
NCOEF = 11
PAD = 8
PIECES = 4
STRIP = 4

VMEM = pltpu.VMEM
SMEM = pltpu.SMEM
HBM = pltpu.HBM


CORNER = [HALO - 2 * ((min(x + 1, HALO - x) + 1) // 2) for x in range(HALO)]


def mode_basis(total, cores):
    theta = np.arange(total)
    wave = []
    for m in range(NM):
        wave.append((m, 0))
    wave.append((total // 2, 0))
    for m in range(1, NM):
        wave.append((m, 1))
    for m in range(NM, total // 2):
        wave.append((m, 0))
        wave.append((m, 1))
    rows, turns = [], []
    for m, kind in wave:
        angle = 2.0 * math.pi * ((m * theta) % total) / total
        row = np.sin(angle) if kind else np.cos(angle)
        norm = 1.0 / total if m in (0, total // 2) else 2.0 / total
        rows.append(row * math.sqrt(norm))
        turns.append(2.0 * math.pi * m / total)
    basis = np.stack(rows).reshape(cores, total // cores, total)
    turns = np.array(turns)
    eigen = (32.0 * np.cos(turns) - 2.0 * np.cos(2.0 * turns) - 30.0) / 12.0
    return basis, eigen.reshape(cores, total // cores)


def split_const(table):
    table = np.asarray(table, np.float32)
    high = table.astype(jnp.bfloat16)
    low = (table - high.astype(np.float32)).astype(jnp.bfloat16)
    return np.stack([high, low])


def halves(x):
    high = x.astype(jnp.bfloat16)
    return high, (x - high.astype(jnp.float32)).astype(jnp.bfloat16)


def dot3(high, low, table_high, table_low):
    dot = functools.partial(jnp.dot, preferred_element_type=jnp.float32)
    return dot(high, table_high) + (dot(low, table_high) + dot(high, table_low))


def position(sizes):
    gx, row, core = lax.axis_index("gx"), lax.axis_index("row"), lax.axis_index("ta")
    share = sizes["row"] // sizes["ta"]
    return gx, row, core, (core - row // share + sizes["ta"]) % sizes["ta"]


def stage_kernel(sizes, own_ref, table_ref, part_ref):
    fields, cx, cr, ct = own_ref.shape
    _, _, core, group = position(sizes)
    for f in range(fields):
        x = own_ref[f].reshape(cx * cr, ct)
        v = dot3(*halves(x), table_ref[0, group, core], table_ref[1, group, core])
        part_ref[:, f] = v.reshape(cx, cr, ct)


def forward_kernel(sizes, first, count, last, part_ref, table_ref, *refs):
    peers, cores = sizes["row"], sizes["ta"]
    sources, refs = refs[: cores - 1], refs[cores - 1 :]
    fields, cx, cr, ct = sources[0].shape
    _, row, core, group = position(sizes)
    step = cx // PIECES
    done = ()
    if last:
        done, refs = refs[:first], refs[first:]
    out = refs[:count]
    for f in range(fields):
        v = part_ref[first * step : (first + count) * step, f].reshape(count * step * cr, ct)
        for k, s in enumerate(sources):
            x = s[f, first * step : (first + count) * step].reshape(count * step * cr, ct)
            other = (core + k + 1) % cores
            v = v + dot3(*halves(x), table_ref[0, group, other], table_ref[1, group, other])
        v = v.reshape(count, step, cr, ct)
        for i in range(count):
            out[i][:, f] = v[i]
    if last:
        e0_ref, eu_ref = refs[count:]
        at = 0
        for i, ref in enumerate(tuple(done) + tuple(out)):
            for side in range(e0_ref.shape[0]):
                top = 1 - row if peers == 2 else 1 - side
                rows = pl.ds(pl.multiple_of((cr - HALO) * top, 8), HALO)
                e0_ref[side, i * step : (i + 1) * step] = ref[:, :, rows]
            for j in range(step):
                n = CORNER[i * step + j]
                for side in range(e0_ref.shape[0]):
                    top = 1 - row if peers == 2 else 1 - side
                    eu_ref[side, :, at : at + n] = ref[j, :, pl.ds((cr - n) * top, n)]
                at += n


def prepare_kernel(
    sizes, cx, cr, rate_ref, speed_ref, mix_ref, cell_ref, owner_ref, eigen_ref,
    coef_ref, place_ref, slots_ref, count_ref,
):
    peers = sizes["row"]
    fields = coef_ref.shape[0]
    shape = coef_ref.shape[2:]
    gx, row, _, group = position(sizes)
    eigen = eigen_ref[group]
    for f in range(fields):
        rate, speed = rate_ref[f], speed_ref[f]
        for g in range(fields):
            value = jnp.full(shape, mix_ref[f, g])
            if g == f:
                value = value + (1.0 + rate * (eigen - 5.0))
            coef_ref[f, g] = value
        line = [
            rate * (16.0 / 12.0),
            rate * (-1.0 / 12.0),
            (16.0 * rate - 8.0 * speed) * (1.0 / 12.0),
            (16.0 * rate + 8.0 * speed) * (1.0 / 12.0),
            (speed - rate) * (1.0 / 12.0),
            (speed + rate) * (-1.0 / 12.0),
        ]
        for i, value in enumerate(line):
            coef_ref[f, fields + i] = jnp.full(shape, value)
    slots_ref[...] = jnp.zeros_like(slots_ref)
    for o in range(peers):
        count_ref[o] = 0
    cells = lax.broadcasted_iota(jnp.int32, (1, cx * cr), 1)

    def station(s, carry):
        owner, cell = owner_ref[s], cell_ref[s]
        rank = count_ref[owner]
        count_ref[owner] = rank + 1
        slot = (owner - row + peers) % peers * CAP + rank
        here = (cell // (cr * peers) - gx * cx) * cr + cell % (cr * peers) - row * cr
        slots_ref[pl.ds(slot, 1)] = (cells == here).astype(jnp.float32)
        return carry

    lax.fori_loop(0, cell_ref.shape[0], station, 0)
    place_ref[...] = slots_ref[...].astype(jnp.bfloat16)


class Frame:
    def __init__(self, sizes, cx, cr, work_ref):
        self.peers, self.cx, self.cr = sizes["row"], cx, cr
        self.fields, self.lanes = work_ref.shape[1], work_ref.shape[3]
        self.rows = work_ref.shape[2] - 2 * PAD
        self.blocks = self.rows // 8
        gx, self.row, self.core, self.group = position(sizes)
        self.odd = gx % 2
        self.even = 1 - self.odd
        self.left = (gx > 0).astype(jnp.int32)
        self.right = (gx < sizes["gx"] - 1).astype(jnp.int32)
        self.sides = 1 if self.peers == 2 else 2
        self.own = PAD + HALO * self.row if self.peers == 2 else PAD + HALO
        if self.peers == 2:
            self.own = pl.multiple_of(self.own, 8)
        self.pair_at = 2 * cx * self.even
        self.far_at = 2 * cx * self.odd

    def halo(self, side, n=HALO):
        if self.peers == 2:
            return PAD + self.row * (HALO - n) + self.cr * (1 - self.row)
        return self.own - n if side == 0 else self.own + self.cr

    def clear(self, low, high, *works):
        zero = jnp.zeros((PAD, self.lanes), jnp.float32)

        def one(x, carry):
            for f in range(self.fields):
                for w in works:
                    w[x, f, pl.ds(0, PAD)] = zero
                    w[x, f, pl.ds(PAD + self.rows, PAD)] = zero
            return carry

        lax.fori_loop(low, high, one, 0)

    def blank(self, low, high, work):
        zero = jnp.zeros((8, self.lanes), jnp.float32)

        def one(x, carry):
            for f in range(self.fields):
                for b in range(self.blocks):
                    work[x, f, pl.ds(PAD + 8 * b, 8)] = zero
            return carry

        lax.fori_loop(low, high, one, 0)

    def place(self, source, work, at, r, low=0, high=None):
        h = source.shape[2]

        def one(i, carry):
            for f in range(self.fields):
                work[at + i, f, pl.ds(r, h)] = source[i, f]
            return carry

        lax.fori_loop(low, source.shape[0] if high is None else high, one, 0)

    def place_edge(self, edge_ref, work, at):
        for side in range(self.sides):
            self.place(edge_ref.at[side], work, at, pl.multiple_of(self.halo(side), 8))

    def place_corner(self, corner_ref, work, at):
        for side in range(self.sides):
            row = 0
            for x, n in enumerate(CORNER):
                work[at + x, :, pl.ds(self.halo(side, n), n)] = corner_ref[side, :, row : row + n]
                row += n

    def layer(self, coef_ref, src, store, x, base, count):
        fields = self.fields
        v = [[src[x, f, pl.ds(base + 8 * b, 8)] for b in range(count)] for f in range(fields)]
        for f in range(fields):
            c = [coef_ref[f, i] for i in range(NCOEF)]
            for b in range(count):
                r = base + 8 * b
                total = c[0] * v[0][b]
                for g in range(1, fields):
                    total = total + c[g] * v[g][b]
                near = src[x, f, pl.ds(r + 1, 8)] + src[x, f, pl.ds(r - 1, 8)]
                far = src[x, f, pl.ds(r + 2, 8)] + src[x, f, pl.ds(r - 2, 8)]
                side = c[fields] * near + c[fields + 1] * far
                one = c[fields + 2] * src[x + 1, f, pl.ds(r, 8)] + c[fields + 3] * src[x - 1, f, pl.ds(r, 8)]
                two = c[fields + 4] * src[x + 2, f, pl.ds(r, 8)] + c[fields + 5] * src[x - 2, f, pl.ds(r, 8)]
                store(x, f, b, (total + side) + (one + two))

    def sweep(self, coef_ref, src, dst, low, high):
        def store(x, f, b, value):
            dst[x, f, pl.ds(PAD + 8 * b, 8)] = value

        def body(x, carry):
            self.layer(coef_ref, src, store, x, PAD, self.blocks)
            return carry

        lax.fori_loop(low, high, body, 0)
        if self.peers > 2:
            for side, edge in ((0, 0), (1, self.peers - 1)):

                @pl.when(self.row == edge)
                def _(side=side):
                    def wipe(x, carry):
                        for f in range(self.fields):
                            dst[x, f, pl.ds(self.halo(side), HALO)] = jnp.zeros(
                                (HALO, self.lanes), jnp.float32
                            )
                        return carry

                    lax.fori_loop(low, high, wipe, 0)

    def pressure(self, weight_ref, p_ref, t, read, low, high):
        def one(x, carry):
            for b in range(self.cr // 8):
                p = weight_ref[0] * read(x, 0, 8 * b)
                for f in range(1, self.fields):
                    p = p + weight_ref[f] * read(x, f, 8 * b)
                p_ref[t, pl.ds(pl.multiple_of((x - self.cx) * self.cr + 8 * b, 8), 8)] = p
            return carry

        lax.fori_loop(low, high, one, 0)


def near_kernel(sizes, coef_ref, weight_ref, *refs):
    own_refs, pair_refs = refs[:PIECES], refs[PIECES : 2 * PIECES]
    r0_ref, rp_ref, strip_ref, p_ref, w0_ref, w1_ref = refs[2 * PIECES :]
    step, cr = own_refs[0].shape[0], own_refs[0].shape[2]
    cx = step * PIECES
    z = Frame(sizes, cx, cr, w0_ref)
    first = cx * z.even
    z.clear(first, first + 2 * cx, w0_ref, w1_ref)
    for i in range(PIECES):
        z.place(own_refs[i], w0_ref, cx + i * step, z.own)
        z.place(pair_refs[i], w0_ref, z.pair_at + i * step, z.own)
    z.place_edge(r0_ref, w0_ref, cx)
    z.place_corner(rp_ref, w0_ref, z.pair_at)
    p_ref[...] = jnp.zeros_like(p_ref)
    works = [w0_ref, w1_ref]
    for t in range(1, STEPS):
        src, dst = works[(t - 1) % 2], works[t % 2]
        low = (cx + 2 * t) * z.even + 2 * t * z.odd
        high = (3 * cx - 2 * t) * z.even + (2 * cx - 2 * t) * z.odd
        z.sweep(coef_ref, src, dst, low, high)
        edge = low * z.even + (high - STRIP) * z.odd
        for i in range(STRIP):
            strip_ref[t - 1, i] = dst[edge + i, :, pl.ds(PAD, z.rows)]
        z.pressure(
            weight_ref, p_ref, t - 1,
            lambda x, f, r, dst=dst: dst[x, f, pl.ds(z.own + r, 8)],
            cx + 2 * t * z.even, 2 * cx - 2 * t * z.odd,
        )


def far_kernel(sizes, coef_ref, weight_ref, place_ref, *refs):
    own_refs, far_refs = refs[:PIECES], refs[PIECES : 2 * PIECES]
    r0_ref, rc_ref, strip_ref, part_ref, out_ref = refs[2 * PIECES : 2 * PIECES + 5]
    cycle_refs = refs[2 * PIECES + 5 : -3]
    w0_ref, w1_ref, p_ref = refs[-3:]
    step, cr = own_refs[0].shape[0], own_refs[0].shape[2]
    cx = step * PIECES
    z = Frame(sizes, cx, cr, w0_ref)
    first = cx * z.odd
    z.clear(first, first + 2 * cx, w0_ref, w1_ref)
    for i in range(PIECES):
        z.place(own_refs[i], w0_ref, cx + i * step, z.own)
        z.place(far_refs[i], w0_ref, z.far_at + i * step, z.own)
    z.place_edge(r0_ref, w0_ref, cx)
    z.place_corner(rc_ref, w0_ref, z.far_at)
    z.blank(cx - 2, cx - 2 + 2 * (1 - z.left), w1_ref)
    z.blank(2 * cx, 2 * cx + 2 * (1 - z.right), w1_ref)
    works = [w0_ref, w1_ref]
    for t in range(1, STEPS):
        src, dst = works[(t - 1) % 2], works[t % 2]
        reach = HALO - 2 * t
        low = (cx - reach * z.left) * z.even + (2 * cx - 2 * t) * z.odd
        high = (cx + 2 * t) * z.even + (2 * cx + reach * z.right) * z.odd
        z.sweep(coef_ref, src, dst, low, high)
        edge = (cx + 2 * t) * z.even + (2 * cx - 2 * t - STRIP) * z.odd
        for i in range(STRIP):
            dst[edge + i, :, pl.ds(PAD, z.rows)] = strip_ref[t - 1, i]
        p_ref[t - 1] = part_ref[t - 1]
        z.pressure(
            weight_ref, p_ref, t - 1,
            lambda x, f, r, dst=dst: dst[x, f, pl.ds(z.own + r, 8)],
            cx * z.even + (2 * cx - 2 * t) * z.odd, (cx + 2 * t) * z.even + 2 * cx * z.odd,
        )
    src = works[(STEPS - 1) % 2]

    def store_out(x, f, b, value):
        out_ref[x - cx, f, pl.ds(8 * b, 8)] = value

    def body_out(x, carry):
        z.layer(coef_ref, src, store_out, x, z.own, cr // 8)
        return carry

    lax.fori_loop(cx, 2 * cx, body_out, 0)
    z.pressure(weight_ref, p_ref, STEPS - 1, lambda x, f, r: out_ref[x - cx, f, pl.ds(r, 8)], cx, 2 * cx)
    dot = functools.partial(jnp.dot, preferred_element_type=jnp.float32)
    for t in range(STEPS):
        high, low = halves(p_ref[t])
        picked = dot(place_ref[...], high) + dot(place_ref[...], low)
        for k, ref in enumerate(cycle_refs):
            ref[t] = picked[k * CAP : (k + 1) * CAP]


def inverse_kernel(sizes, *refs):
    cores = sizes["ta"]
    sources = refs[:cores]
    table_ref, out_ref, x_ref, sems = refs[cores:]
    fields, cx, cr, ct = out_ref.shape
    _, _, core, group = position(sizes)
    table = [
        jnp.concatenate([table_ref[i, (group + k) % cores, core] for k in range(cores)], axis=0)
        for i in range(2)
    ]
    copies = []
    for f in range(fields):
        x = jnp.concatenate([s[:, f].reshape(cx * cr, ct) for s in sources], axis=1)
        x_ref[f] = dot3(*halves(x), *table).reshape(cx, cr, ct)
        copies.append(pltpu.make_async_copy(x_ref.at[f], out_ref.at[f], sems.at[f]))
        copies[f].start()
    for copy in copies:
        copy.wait()


def spectra_kernel(sizes, *refs):
    peers = sizes["row"]
    received = refs[:peers]
    window_ref, out_ref = refs[peers:]
    _, row, core, _ = position(sizes)
    share = peers // sizes["ta"]
    blocks = []
    for j in range(share):
        hop = (row - (core * share + j) + peers) % peers
        value = jnp.where(hop == 0, received[0][...], 0.0)
        for k in range(1, peers):
            value = jnp.where(hop == k, received[k][...], value)
        blocks.append(value)
    x = blocks[0] if share == 1 else jnp.concatenate(blocks, axis=1)
    lane = lax.broadcasted_iota(jnp.int32, (1, x.shape[2]), 1)
    scale = jnp.where(lane == 0, 1.0, math.sqrt(0.5))
    keep = jnp.where(lane == 0, 0.0, math.sqrt(0.5))
    cosine, sine = [], []
    for t in range(STEPS):
        value = x[t] * (window_ref[t].astype(jnp.float32) * 0.125)
        cosine.append(value * scale)
        sine.append(pltpu.roll(value, x.shape[2] - NM, 1) * keep)
    for k in range(NFREQ):
        real = imag = None
        for t in range(STEPS):
            phase = math.pi * t * (k + 1) / NFREQ
            c, s = math.cos(phase), math.sin(phase)
            re = cosine[t] if t == 0 else c * cosine[t] - s * sine[t]
            im = -sine[t] if t == 0 else -s * cosine[t] - c * sine[t]
            real = re if real is None else real + re
            imag = im if imag is None else imag + im
        out_ref[0, :, 2 * k * NM : (2 * k + 1) * NM] = real[:, :NM]
        out_ref[0, :, (2 * k + 1) * NM : (2 * k + 2) * NM] = imag[:, :NM]


def spec(space, n):
    return [pl.BlockSpec(memory_space=space)] * n


def limit(mib):
    return pltpu.CompilerParams(vmem_limit_bytes=mib << 20)


def work_for(flops):
    return pl.CostEstimate(flops=flops, bytes_accessed=10**6, transcendentals=0)


def local(
    sizes,
    conserved,
    diffusivity,
    axial_speed,
    coupling,
    pressure_weights,
    station_cell,
    owner_row,
    window_table,
):
    fields, cx, cr, ct = conserved.shape
    nx, peers, cores = sizes["gx"], sizes["row"], sizes["ta"]
    assert cx == HALO and nx % 2 == 0 and peers % cores == 0
    share = peers // cores
    step = cx // PIECES
    sides = 1 if peers == 2 else 2
    basis, eigen = mode_basis(ct * cores, cores)
    blocks = basis.reshape(cores, ct, cores, ct).transpose(0, 2, 3, 1)
    ahead = split_const(blocks)
    back = split_const(blocks.transpose(0, 1, 3, 2))

    def shape(*dims):
        return jax.ShapeDtypeStruct(dims, jnp.float32)

    def others(x):
        return [
            lax.ppermute(x, "ta", [((c + k) % cores, c) for c in range(cores)])
            for k in range(1, cores)
        ]

    sources = others(conserved)
    part = pl.pallas_call(
        functools.partial(stage_kernel, sizes),
        out_shape=shape(cx, fields, cr, ct),
        in_specs=spec(VMEM, 2),
        out_specs=pl.BlockSpec(memory_space=VMEM),
        compiler_params=limit(8),
        cost_estimate=work_for(10**7),
        name="stage",
    )(conserved, ahead)
    tile = shape(step, fields, cr, ct)
    edge = shape(sides, cx, fields, HALO, ct)
    early = PIECES // 2
    own = list(
        pl.pallas_call(
            functools.partial(forward_kernel, sizes, 0, early, False),
            out_shape=(tile,) * early,
            in_specs=spec(VMEM, cores + 1),
            out_specs=tuple(spec(VMEM, early)),
            compiler_params=limit(8),
            cost_estimate=work_for(10**6),
            name="forward_early",
        )(part, ahead, *sources)
    )
    *rest, e0, eu = pl.pallas_call(
        functools.partial(forward_kernel, sizes, early, PIECES - early, True),
        out_shape=(tile,) * (PIECES - early) + (edge, shape(sides, fields, sum(CORNER), ct)),
        in_specs=spec(VMEM, cores + 1 + early),
        out_specs=tuple(spec(VMEM, PIECES - early + 2)),
        compiler_params=limit(8),
        cost_estimate=work_for(10**6),
        name="forward_late",
    )(part, ahead, *sources, *own)
    own += rest

    swap = [(i, i ^ 1) for i in range(nx)]
    onward = [(i, i + 2 if i % 2 == 0 else i - 2) for i in range(nx)]
    onward = [(a, b) for a, b in onward if 0 <= b < nx]

    def radial(x):
        got = []
        for side in range(sides):
            if peers == 2:
                turn = [(0, 1), (1, 0)]
            else:
                turn = [(r, r + 1) for r in range(peers - 1)]
                if side:
                    turn = [(b, a) for a, b in turn]
            hops = [
                (r * cores + (g + r // share) % cores, q * cores + (g + q // share) % cores)
                for r, q in turn
                for g in range(cores)
            ]
            got.append(lax.ppermute(x[side : side + 1], ("row", "ta"), hops))
        return got[0] if sides == 1 else jnp.concatenate(got, axis=0)

    r0 = radial(e0)
    ru = radial(eu)
    pair, far = [], []
    for x in own:
        pair.append(lax.ppermute(x, "gx", swap))
    rp = lax.ppermute(ru, "gx", swap)
    rc = lax.ppermute(rp, "gx", onward)
    for x in pair:
        far.append(lax.ppermute(x, "gx", onward))

    lines = np.broadcast_to(eigen[:, None, :], (cores, 8, ct)).astype(np.float32)
    coef, place = pl.pallas_call(
        functools.partial(prepare_kernel, sizes, cx, cr),
        out_shape=(
            shape(fields, NCOEF, 8, ct),
            jax.ShapeDtypeStruct((peers * CAP, cx * cr), jnp.bfloat16),
        ),
        in_specs=spec(SMEM, 5) + spec(VMEM, 1),
        out_specs=tuple(spec(VMEM, 2)),
        scratch_shapes=[
            pltpu.VMEM((peers * CAP, cx * cr), jnp.float32),
            pltpu.SMEM((peers,), jnp.int32),
        ],
        compiler_params=limit(4),
        cost_estimate=work_for(10**6),
        name="prepare",
    )(diffusivity, axial_speed, coupling, station_cell, owner_row.reshape(-1), lines)

    rows = cr + HALO * sides
    work = pltpu.VMEM((3 * cx, fields, rows + 2 * PAD, ct), jnp.float32)
    strip, parts = pl.pallas_call(
        functools.partial(near_kernel, sizes),
        out_shape=(shape(STEPS - 1, STRIP, fields, rows, ct), shape(STEPS - 1, cx * cr, ct)),
        in_specs=spec(VMEM, 1) + spec(SMEM, 1) + spec(VMEM, 2 * PIECES + 2),
        out_specs=tuple(spec(VMEM, 2)),
        scratch_shapes=[work, work],
        compiler_params=limit(20),
        cost_estimate=work_for(10**7),
        name="near",
    )(coef, pressure_weights, *own, *pair, r0, rp)
    modes, *cycles = pl.pallas_call(
        functools.partial(far_kernel, sizes),
        out_shape=(shape(cx, fields, cr, ct),) + (shape(STEPS, CAP, ct),) * peers,
        in_specs=spec(VMEM, 1) + spec(SMEM, 1) + spec(VMEM, 1 + 2 * PIECES + 4),
        out_specs=tuple(spec(VMEM, 1 + peers)),
        scratch_shapes=[work, work, pltpu.VMEM((STEPS, cx * cr, ct), jnp.float32)],
        compiler_params=limit(20),
        cost_estimate=work_for(10**7),
        name="rest",
    )(coef, pressure_weights, place, *own, *far, r0, rc, strip, parts)

    received = [cycles[0]]
    for k in range(1, peers):
        pairs = []
        for j in range(peers):
            pairs.append((j * cores + j // share, (j + k) % peers * cores + j // share))
        received.append(lax.ppermute(cycles[k], ("row", "ta"), pairs))

    advanced = pl.pallas_call(
        functools.partial(inverse_kernel, sizes),
        out_shape=jax.ShapeDtypeStruct(conserved.shape, jnp.float32),
        in_specs=spec(VMEM, cores + 1),
        out_specs=pl.BlockSpec(memory_space=HBM),
        scratch_shapes=[pltpu.VMEM(conserved.shape, jnp.float32), pltpu.SemaphoreType.DMA((fields,))],
        compiler_params=limit(8),
        cost_estimate=work_for(10**6),
        name="inverse",
    )(modes, *others(modes), back)
    spectra = pl.pallas_call(
        functools.partial(spectra_kernel, sizes),
        out_shape=shape(1, share * CAP, NFREQ * 2 * NM),
        in_specs=spec(VMEM, peers) + spec(SMEM, 1),
        out_specs=pl.BlockSpec(memory_space=VMEM),
        compiler_params=limit(8),
        cost_estimate=work_for(10**6),
        name="spectra",
    )(*received, window_table)
    return (advanced, spectra)


def solution(mesh):
    in_specs = (
        P(None, "gx", "row", "ta"),
        P(),
        P(),
        P(),
        P(),
        P(("gx", "row")),
        P(("gx", "row"), None),
        P(),
    )
    out_specs = (P(None, "gx", "row", "ta"), P(("gx", "row"), "ta", None))

    def body(*args):
        return local(dict(mesh.shape), *args)

    return jax.shard_map(body, mesh=mesh, in_specs=in_specs, out_specs=out_specs, check_vma=False)
```

```python
import functools
import math

import jax
import jax.numpy as jnp
import numpy as np
from jax import lax
from jax.experimental import pallas as pl
from jax.experimental.pallas import tpu as pltpu
from jax.sharding import PartitionSpec as P


NM = 33
NFREQ = 16
STEPS = 4
CAP = 16
HALO = 2 * STEPS
NCOEF = 11
PAD = 8
PIECES = 4
NEAR_PIECES = 2

VMEM = pltpu.VMEM
SMEM = pltpu.SMEM
HBM = pltpu.HBM


CORNER = [HALO - 2 * ((min(x + 1, HALO - x) + 1) // 2) for x in range(HALO)]


def mode_basis(total, cores):
    theta = np.arange(total)
    wave = []
    for m in range(NM):
        wave.append((m, 0))
    wave.append((total // 2, 0))
    for m in range(1, NM):
        wave.append((m, 1))
    for m in range(NM, total // 2):
        wave.append((m, 0))
        wave.append((m, 1))
    rows, turns = [], []
    for m, kind in wave:
        angle = 2.0 * math.pi * ((m * theta) % total) / total
        row = np.sin(angle) if kind else np.cos(angle)
        norm = 1.0 / total if m in (0, total // 2) else 2.0 / total
        rows.append(row * math.sqrt(norm))
        turns.append(2.0 * math.pi * m / total)
    basis = np.stack(rows).reshape(cores, total // cores, total)
    turns = np.array(turns)
    eigen = (32.0 * np.cos(turns) - 2.0 * np.cos(2.0 * turns) - 30.0) / 12.0
    return basis, eigen.reshape(cores, total // cores)


def split_const(table):
    table = np.asarray(table, np.float32)
    high = table.astype(jnp.bfloat16)
    low = (table - high.astype(np.float32)).astype(jnp.bfloat16)
    return np.stack([high, low])


def halves(x):
    high = x.astype(jnp.bfloat16)
    return high, (x - high.astype(jnp.float32)).astype(jnp.bfloat16)


def dot3(high, low, table_high, table_low):
    dot = functools.partial(jnp.dot, preferred_element_type=jnp.float32)
    return dot(high, table_high) + (dot(low, table_high) + dot(high, table_low))


def position(sizes):
    gx, row, core = lax.axis_index("gx"), lax.axis_index("row"), lax.axis_index("ta")
    share = sizes["row"] // sizes["ta"]
    return gx, row, core, (core - row // share + sizes["ta"]) % sizes["ta"]


def stage_kernel(sizes, own_ref, table_ref, part_ref):
    fields, cx, cr, ct = own_ref.shape
    _, _, core, group = position(sizes)
    for f in range(fields):
        x = own_ref[f].reshape(cx * cr, ct)
        v = dot3(*halves(x), table_ref[0, group, core], table_ref[1, group, core])
        part_ref[:, f] = v.reshape(cx, cr, ct)


def forward_kernel(sizes, first, count, last, part_ref, table_ref, *refs):
    peers, cores = sizes["row"], sizes["ta"]
    sources, refs = refs[: cores - 1], refs[cores - 1 :]
    fields, cx, cr, ct = sources[0].shape
    gx, row, core, group = position(sizes)
    odd = gx % 2
    step = cx // PIECES
    low = step * (first + (PIECES - 2 * first - count) * odd)
    done = ()
    if last:
        done, refs = refs[:first], refs[first:]
    out = refs[:count]
    for f in range(fields):
        v = part_ref[pl.ds(low, count * step), f].reshape(count * step * cr, ct)
        for k, s in enumerate(sources):
            x = s[f, pl.ds(low, count * step)].reshape(count * step * cr, ct)
            other = (core + k + 1) % cores
            v = v + dot3(*halves(x), table_ref[0, group, other], table_ref[1, group, other])
        v = v.reshape(count, step, cr, ct)
        for i in range(count):
            out[i][:, f] = jnp.where(odd == 1, v[count - 1 - i], v[i])
    if last:
        e0_ref, eu_ref = refs[count:]
        starts = [sum(CORNER[:x]) for x in range(cx)]
        for i, ref in enumerate(tuple(done) + tuple(out)):
            block = i + (PIECES - 1 - 2 * i) * odd
            mirror = step * (PIECES - 1 - i)
            for side in range(e0_ref.shape[0]):
                top = 1 - row if peers == 2 else 1 - side
                rows = pl.ds(pl.multiple_of((cr - HALO) * top, 8), HALO)
                e0_ref[side, pl.ds(block * step, step)] = ref[:, :, rows]
                for j in range(step):
                    n = CORNER[i * step + j]
                    at = starts[i * step + j]
                    at = at + (starts[mirror + j] - at) * odd
                    eu_ref[side, :, pl.ds(at, n)] = ref[j, :, pl.ds((cr - n) * top, n)]


def prepare_kernel(
    sizes, cx, cr, rate_ref, speed_ref, mix_ref, cell_ref, owner_ref, eigen_ref,
    coef_ref, place_ref, slots_ref, count_ref,
):
    peers = sizes["row"]
    fields = coef_ref.shape[0]
    shape = coef_ref.shape[2:]
    gx, row, _, group = position(sizes)
    eigen = eigen_ref[group]
    for f in range(fields):
        rate, speed = rate_ref[f], speed_ref[f]
        for g in range(fields):
            value = jnp.full(shape, mix_ref[f, g])
            if g == f:
                value = value + (1.0 + rate * (eigen - 5.0))
            coef_ref[f, g] = value
        line = [
            rate * (16.0 / 12.0),
            rate * (-1.0 / 12.0),
            (16.0 * rate - 8.0 * speed) * (1.0 / 12.0),
            (16.0 * rate + 8.0 * speed) * (1.0 / 12.0),
            (speed - rate) * (1.0 / 12.0),
            (speed + rate) * (-1.0 / 12.0),
        ]
        for i, value in enumerate(line):
            coef_ref[f, fields + i] = jnp.full(shape, value)
    slots_ref[...] = jnp.zeros_like(slots_ref)
    for o in range(peers):
        count_ref[o] = 0
    cells = lax.broadcasted_iota(jnp.int32, (1, cx * cr), 1)

    def station(s, carry):
        owner, cell = owner_ref[s], cell_ref[s]
        rank = count_ref[owner]
        count_ref[owner] = rank + 1
        slot = (owner - row + peers) % peers * CAP + rank
        here = (cell // (cr * peers) - gx * cx) * cr + cell % (cr * peers) - row * cr
        slots_ref[pl.ds(slot, 1)] = (cells == here).astype(jnp.float32)
        return carry

    lax.fori_loop(0, cell_ref.shape[0], station, 0)
    place_ref[...] = slots_ref[...].astype(jnp.bfloat16)


class Frame:
    def __init__(self, sizes, cx, cr, work_ref):
        self.peers, self.cx, self.cr = sizes["row"], cx, cr
        self.fields, self.lanes = work_ref.shape[1], work_ref.shape[3]
        self.rows = work_ref.shape[2] - 2 * PAD
        self.blocks = self.rows // 8
        gx, self.row, self.core, self.group = position(sizes)
        self.odd = gx % 2
        self.even = 1 - self.odd
        self.left = (gx > 0).astype(jnp.int32)
        self.right = (gx < sizes["gx"] - 1).astype(jnp.int32)
        self.sides = 1 if self.peers == 2 else 2
        self.own = PAD + HALO * self.row if self.peers == 2 else PAD + HALO
        if self.peers == 2:
            self.own = pl.multiple_of(self.own, 8)
        self.pair_at = 2 * cx * self.even
        self.far_at = 2 * cx * self.odd

    def block(self, piece, odd):
        return piece + (PIECES - 1 - 2 * piece) * odd

    def tile(self, work):
        return lambda x, f, r: work[x, f, pl.ds(self.own + r, 8)]

    def halo(self, side, n=HALO):
        if self.peers == 2:
            return PAD + self.row * (HALO - n) + self.cr * (1 - self.row)
        return self.own - n if side == 0 else self.own + self.cr

    def clear(self, low, high, *works):
        zero = jnp.zeros((PAD, self.lanes), jnp.float32)

        def one(x, carry):
            for f in range(self.fields):
                for w in works:
                    w[x, f, pl.ds(0, PAD)] = zero
                    w[x, f, pl.ds(PAD + self.rows, PAD)] = zero
            return carry

        lax.fori_loop(low, high, one, 0)

    def blank(self, low, high, work):
        zero = jnp.zeros((8, self.lanes), jnp.float32)

        def one(x, carry):
            for f in range(self.fields):
                for b in range(self.blocks):
                    work[x, f, pl.ds(PAD + 8 * b, 8)] = zero
            return carry

        lax.fori_loop(low, high, one, 0)

    def place(self, source, work, at, r, low=0, high=None):
        h = source.shape[2]

        def one(i, carry):
            for f in range(self.fields):
                work[at + i, f, pl.ds(r, h)] = source[i, f]
            return carry

        lax.fori_loop(low, source.shape[0] if high is None else high, one, 0)

    def place_edge(self, edge_ref, work, at):
        for side in range(self.sides):
            self.place(edge_ref.at[side], work, at, pl.multiple_of(self.halo(side), 8))

    def place_corner(self, corner_ref, work, at):
        for side in range(self.sides):
            row = 0
            for x, n in enumerate(CORNER):
                work[at + x, :, pl.ds(self.halo(side, n), n)] = corner_ref[side, :, row : row + n]
                row += n

    def layer(self, coef_ref, src, store, x, base, count):
        fields = self.fields
        v = [[src[x, f, pl.ds(base + 8 * b, 8)] for b in range(count)] for f in range(fields)]
        for f in range(fields):
            c = [coef_ref[f, i] for i in range(NCOEF)]
            for b in range(count):
                r = base + 8 * b
                total = c[0] * v[0][b]
                for g in range(1, fields):
                    total = total + c[g] * v[g][b]
                near = src[x, f, pl.ds(r + 1, 8)] + src[x, f, pl.ds(r - 1, 8)]
                far = src[x, f, pl.ds(r + 2, 8)] + src[x, f, pl.ds(r - 2, 8)]
                side = c[fields] * near + c[fields + 1] * far
                one = c[fields + 2] * src[x + 1, f, pl.ds(r, 8)] + c[fields + 3] * src[x - 1, f, pl.ds(r, 8)]
                two = c[fields + 4] * src[x + 2, f, pl.ds(r, 8)] + c[fields + 5] * src[x - 2, f, pl.ds(r, 8)]
                store(x, f, b, (total + side) + (one + two))

    def sweep(self, coef_ref, src, dst, low, high):
        def store(x, f, b, value):
            dst[x, f, pl.ds(PAD + 8 * b, 8)] = value

        def body(x, carry):
            self.layer(coef_ref, src, store, x, PAD, self.blocks)
            return carry

        lax.fori_loop(low, high, body, 0)
        if self.peers > 2:
            for side, edge in ((0, 0), (1, self.peers - 1)):

                @pl.when(self.row == edge)
                def _(side=side):
                    def wipe(x, carry):
                        for f in range(self.fields):
                            dst[x, f, pl.ds(self.halo(side), HALO)] = jnp.zeros(
                                (HALO, self.lanes), jnp.float32
                            )
                        return carry

                    lax.fori_loop(low, high, wipe, 0)

    def pressure(self, weight_ref, p_ref, t, read, low, count):
        for i in range(count):
            x = low + i
            for b in range(self.cr // 8):
                p = weight_ref[0] * read(x, 0, 8 * b)
                for f in range(1, self.fields):
                    p = p + weight_ref[f] * read(x, f, 8 * b)
                p_ref[t, pl.ds(pl.multiple_of((x - self.cx) * self.cr + 8 * b, 8), 8)] = p


def setup_kernel(sizes, *refs):
    own_refs, levels = refs[:PIECES], refs[PIECES:]
    step, cr = own_refs[0].shape[0], own_refs[0].shape[2]
    cx = step * PIECES
    z = Frame(sizes, cx, cr, levels[0])
    for t in range(STEPS):
        z.clear(2 * t + 2, 3 * cx - 2 * t - 2, levels[t])
    for i in range(PIECES):
        z.place(own_refs[i], levels[0], cx + z.block(i, z.odd) * step, z.own)
    for t in range(1, STEPS):
        z.blank(cx - 2, cx - 2 + 2 * (1 - z.left), levels[t])
        z.blank(2 * cx, 2 * cx + 2 * (1 - z.right), levels[t])


def near_kernel(sizes, coef_ref, weight_ref, *refs):
    pair_refs, refs = refs[:PIECES], refs[PIECES:]
    r0_ref, rp_ref, p_ref, *levels = refs[:2] + refs[2 + STEPS :]
    step, cr = pair_refs[0].shape[0], pair_refs[0].shape[2]
    cx = step * PIECES
    z = Frame(sizes, cx, cr, levels[0])
    for i in range(PIECES):
        z.place(pair_refs[i], levels[0], z.pair_at + z.block(i, z.even) * step, z.own)
    z.place_edge(r0_ref, levels[0], cx)
    z.place_corner(rp_ref, levels[0], z.pair_at)
    for t in range(1, STEPS):
        low = (cx + 2 * t) * z.even + 2 * t * z.odd
        z.sweep(coef_ref, levels[t - 1], levels[t], low, low + 2 * cx - 4 * t)
        z.pressure(weight_ref, p_ref, t - 1, z.tile(levels[t]), cx + 2 * t * z.even, cx - 2 * t)


def outward(z, coef_ref, levels, t, reach):
    low = jnp.maximum(z.cx - reach, z.cx - 2 * STEPS * z.left) * z.even
    high = (z.cx - reach + 4) * z.even
    low = low + (2 * z.cx + reach - 4) * z.odd
    high = high + jnp.minimum(2 * z.cx + reach, 2 * z.cx + 2 * STEPS * z.right) * z.odd
    z.sweep(coef_ref, levels[t - 1], levels[t], low, high)


def middle_kernel(sizes, coef_ref, weight_ref, place_ref, *refs):
    far_refs, refs = refs[:NEAR_PIECES], refs[NEAR_PIECES:]
    rc_ref, refs = refs[0], refs[1 + 1 + STEPS :]
    p_ref, levels, pick_ref = refs[0], refs[1 : 1 + STEPS], refs[1 + STEPS]
    step, cr = far_refs[0].shape[0], far_refs[0].shape[2]
    cx = step * PIECES
    z = Frame(sizes, cx, cr, levels[0])
    for i in range(NEAR_PIECES):
        z.place(far_refs[i], levels[0], z.far_at + z.block(i, z.even) * step, z.own)
    z.place_corner(rc_ref, levels[0], z.far_at)
    for t in range(1, STEPS):
        reach = 4 - 2 * t
        outward(z, coef_ref, levels, t, reach)
        count = min(4, 4 - reach) if reach < 4 else 0
        count = min(count, 2 * t)
        low = cx - min(reach, 0)
        z.pressure(weight_ref, p_ref, t - 1, z.tile(levels[t]), low * z.even + (3 * cx - low - count) * z.odd, count)
    for t in range(2):
        pick_ref[t] = picked(place_ref, p_ref[t])


def picked(place_ref, value):
    high, low = halves(value)
    dot = functools.partial(jnp.dot, preferred_element_type=jnp.float32)
    return dot(place_ref[...], high) + dot(place_ref[...], low)


def far_kernel(sizes, coef_ref, weight_ref, place_ref, *refs):
    far_refs, refs = refs[: PIECES - NEAR_PIECES], refs[PIECES - NEAR_PIECES :]
    pick_ref, refs = refs[0], refs[1 + 1 + STEPS :]
    p_ref, levels, out_ref = refs[0], refs[1 : 1 + STEPS], refs[1 + STEPS]
    cycle_refs = refs[2 + STEPS :]
    step, cr = far_refs[0].shape[0], far_refs[0].shape[2]
    cx = step * PIECES
    z = Frame(sizes, cx, cr, levels[0])
    for i in range(NEAR_PIECES, PIECES):
        z.place(far_refs[i - NEAR_PIECES], levels[0], z.far_at + z.block(i, z.even) * step, z.own)
    for t in range(1, STEPS):
        outward(z, coef_ref, levels, t, HALO - 2 * t)
    z.pressure(
        weight_ref, p_ref, STEPS - 2, z.tile(levels[STEPS - 1]), cx * z.even + (2 * cx - 2) * z.odd, 2
    )

    def store_out(x, f, b, value):
        out_ref[x - cx, f, pl.ds(8 * b, 8)] = value

    def body_out(x, carry):
        z.layer(coef_ref, levels[STEPS - 1], store_out, x, z.own, cr // 8)
        return carry

    lax.fori_loop(cx, 2 * cx, body_out, 0)
    z.pressure(weight_ref, p_ref, STEPS - 1, lambda x, f, r: out_ref[x - cx, f, pl.ds(r, 8)], cx, cx)
    for t in range(STEPS):
        value = pick_ref[t] if t < 2 else picked(place_ref, p_ref[t])
        for k, ref in enumerate(cycle_refs):
            ref[t] = value[k * CAP : (k + 1) * CAP]


def inverse_kernel(sizes, *refs):
    cores = sizes["ta"]
    sources = refs[:cores]
    table_ref, out_ref, x_ref, sems = refs[cores:]
    fields, cx, cr, ct = out_ref.shape
    _, _, core, group = position(sizes)
    table = [
        jnp.concatenate([table_ref[i, (group + k) % cores, core] for k in range(cores)], axis=0)
        for i in range(2)
    ]
    copies = []
    for f in range(fields):
        x = jnp.concatenate([s[:, f].reshape(cx * cr, ct) for s in sources], axis=1)
        x_ref[f] = dot3(*halves(x), *table).reshape(cx, cr, ct)
        copies.append(pltpu.make_async_copy(x_ref.at[f], out_ref.at[f], sems.at[f]))
        copies[f].start()
    for copy in copies:
        copy.wait()


def spectra_kernel(sizes, *refs):
    peers = sizes["row"]
    received = refs[:peers]
    window_ref, out_ref = refs[peers:]
    _, row, core, _ = position(sizes)
    share = peers // sizes["ta"]
    blocks = []
    for j in range(share):
        hop = (row - (core * share + j) + peers) % peers
        value = jnp.where(hop == 0, received[0][...], 0.0)
        for k in range(1, peers):
            value = jnp.where(hop == k, received[k][...], value)
        blocks.append(value)
    x = blocks[0] if share == 1 else jnp.concatenate(blocks, axis=1)
    lane = lax.broadcasted_iota(jnp.int32, (1, x.shape[2]), 1)
    scale = jnp.where(lane == 0, 1.0, math.sqrt(0.5))
    keep = jnp.where(lane == 0, 0.0, math.sqrt(0.5))
    cosine, sine = [], []
    for t in range(STEPS):
        value = x[t] * (window_ref[t].astype(jnp.float32) * 0.125)
        cosine.append(value * scale)
        sine.append(pltpu.roll(value, x.shape[2] - NM, 1) * keep)
    for k in range(NFREQ):
        real = imag = None
        for t in range(STEPS):
            phase = math.pi * t * (k + 1) / NFREQ
            c, s = math.cos(phase), math.sin(phase)
            re = cosine[t] if t == 0 else c * cosine[t] - s * sine[t]
            im = -sine[t] if t == 0 else -s * cosine[t] - c * sine[t]
            real = re if real is None else real + re
            imag = im if imag is None else imag + im
        out_ref[0, :, 2 * k * NM : (2 * k + 1) * NM] = real[:, :NM]
        out_ref[0, :, (2 * k + 1) * NM : (2 * k + 2) * NM] = imag[:, :NM]


def spec(space, n):
    return [pl.BlockSpec(memory_space=space)] * n


def limit(mib):
    return pltpu.CompilerParams(vmem_limit_bytes=mib << 20)


def work_for(flops):
    return pl.CostEstimate(flops=flops, bytes_accessed=10**6, transcendentals=0)


def local(
    sizes,
    conserved,
    diffusivity,
    axial_speed,
    coupling,
    pressure_weights,
    station_cell,
    owner_row,
    window_table,
):
    fields, cx, cr, ct = conserved.shape
    nx, peers, cores = sizes["gx"], sizes["row"], sizes["ta"]
    assert cx == HALO and nx % 2 == 0 and peers % cores == 0
    share = peers // cores
    step = cx // PIECES
    sides = 1 if peers == 2 else 2
    basis, eigen = mode_basis(ct * cores, cores)
    blocks = basis.reshape(cores, ct, cores, ct).transpose(0, 2, 3, 1)
    ahead = split_const(blocks)
    back = split_const(blocks.transpose(0, 1, 3, 2))

    def shape(*dims):
        return jax.ShapeDtypeStruct(dims, jnp.float32)

    def others(x):
        return [
            lax.ppermute(x, "ta", [((c + k) % cores, c) for c in range(cores)])
            for k in range(1, cores)
        ]

    sources = others(conserved)
    part = pl.pallas_call(
        functools.partial(stage_kernel, sizes),
        out_shape=shape(cx, fields, cr, ct),
        in_specs=spec(VMEM, 2),
        out_specs=pl.BlockSpec(memory_space=VMEM),
        compiler_params=limit(8),
        cost_estimate=work_for(10**7),
        name="stage",
    )(conserved, ahead)
    tile = shape(step, fields, cr, ct)
    edge = shape(sides, cx, fields, HALO, ct)
    early = PIECES // 2
    own = list(
        pl.pallas_call(
            functools.partial(forward_kernel, sizes, 0, early, False),
            out_shape=(tile,) * early,
            in_specs=spec(VMEM, cores + 1),
            out_specs=tuple(spec(VMEM, early)),
            compiler_params=limit(8),
            cost_estimate=work_for(10**6),
            name="forward_early",
        )(part, ahead, *sources)
    )
    *rest, e0, eu = pl.pallas_call(
        functools.partial(forward_kernel, sizes, early, PIECES - early, True),
        out_shape=(tile,) * (PIECES - early) + (edge, shape(sides, fields, sum(CORNER), ct)),
        in_specs=spec(VMEM, cores + 1 + early),
        out_specs=tuple(spec(VMEM, PIECES - early + 2)),
        compiler_params=limit(8),
        cost_estimate=work_for(10**6),
        name="forward_late",
    )(part, ahead, *sources, *own)
    own += rest

    swap = [(i, i ^ 1) for i in range(nx)]
    onward = [(i, i + 2 if i % 2 == 0 else i - 2) for i in range(nx)]
    onward = [(a, b) for a, b in onward if 0 <= b < nx]

    def radial(x):
        got = []
        for side in range(sides):
            if peers == 2:
                turn = [(0, 1), (1, 0)]
            else:
                turn = [(r, r + 1) for r in range(peers - 1)]
                if side:
                    turn = [(b, a) for a, b in turn]
            hops = [
                (r * cores + (g + r // share) % cores, q * cores + (g + q // share) % cores)
                for r, q in turn
                for g in range(cores)
            ]
            got.append(lax.ppermute(x[side : side + 1], ("row", "ta"), hops))
        return got[0] if sides == 1 else jnp.concatenate(got, axis=0)

    r0 = radial(e0)
    ru = radial(eu)
    pair, far = [], []
    for x in own:
        pair.append(lax.ppermute(x, "gx", swap))
    rp = lax.ppermute(ru, "gx", swap)
    rc = lax.ppermute(rp, "gx", onward)
    for x in pair:
        far.append(lax.ppermute(x, "gx", onward))

    lines = np.broadcast_to(eigen[:, None, :], (cores, 8, ct)).astype(np.float32)
    coef, place = pl.pallas_call(
        functools.partial(prepare_kernel, sizes, cx, cr),
        out_shape=(
            shape(fields, NCOEF, 8, ct),
            jax.ShapeDtypeStruct((peers * CAP, cx * cr), jnp.bfloat16),
        ),
        in_specs=spec(SMEM, 5) + spec(VMEM, 1),
        out_specs=tuple(spec(VMEM, 2)),
        scratch_shapes=[
            pltpu.VMEM((peers * CAP, cx * cr), jnp.float32),
            pltpu.SMEM((peers,), jnp.int32),
        ],
        compiler_params=limit(4),
        cost_estimate=work_for(10**6),
        name="prepare",
    )(diffusivity, axial_speed, coupling, station_cell, owner_row.reshape(-1), lines)

    rows = cr + HALO * sides
    state = (shape(STEPS, cx * cr, ct),) + (shape(3 * cx, fields, rows + 2 * PAD, ct),) * STEPS
    held = len(state)
    levels = pl.pallas_call(
        functools.partial(setup_kernel, sizes),
        out_shape=state[1:],
        in_specs=spec(VMEM, PIECES),
        out_specs=tuple(spec(VMEM, STEPS)),
        compiler_params=limit(20),
        cost_estimate=work_for(10**6),
        name="setup",
    )(*own)
    levels = pl.pallas_call(
        functools.partial(near_kernel, sizes),
        out_shape=state,
        in_specs=spec(VMEM, 1) + spec(SMEM, 1) + spec(VMEM, PIECES + 2 + STEPS),
        out_specs=tuple(spec(VMEM, held)),
        input_output_aliases={4 + PIECES + i: 1 + i for i in range(STEPS)},
        compiler_params=limit(20),
        cost_estimate=work_for(10**7),
        name="near",
    )(coef, pressure_weights, *pair, r0, rp, *levels)
    count = NEAR_PIECES
    *levels, picks = pl.pallas_call(
        functools.partial(middle_kernel, sizes),
        out_shape=state + (shape(2, peers * CAP, ct),),
        in_specs=spec(VMEM, 1) + spec(SMEM, 1) + spec(VMEM, 1 + count + 1 + held),
        out_specs=tuple(spec(VMEM, held + 1)),
        input_output_aliases={4 + count + i: i for i in range(held)},
        compiler_params=limit(20),
        cost_estimate=work_for(10**7),
        name="middle",
    )(coef, pressure_weights, place, *far[:count], rc, *levels)
    results = pl.pallas_call(
        functools.partial(far_kernel, sizes),
        out_shape=state + (shape(cx, fields, cr, ct),) + (shape(STEPS, CAP, ct),) * peers,
        in_specs=spec(VMEM, 1) + spec(SMEM, 1) + spec(VMEM, 1 + PIECES - count + 1 + held),
        out_specs=tuple(spec(VMEM, held + 1 + peers)),
        input_output_aliases={4 + PIECES - count + i: i for i in range(held)},
        compiler_params=limit(20),
        cost_estimate=work_for(10**7),
        name="rest",
    )(coef, pressure_weights, place, *far[count:], picks, *levels)
    modes, cycles = results[held], results[held + 1 :]

    received = [cycles[0]]
    for k in range(1, peers):
        pairs = []
        for j in range(peers):
            pairs.append((j * cores + j // share, (j + k) % peers * cores + j // share))
        received.append(lax.ppermute(cycles[k], ("row", "ta"), pairs))

    advanced = pl.pallas_call(
        functools.partial(inverse_kernel, sizes),
        out_shape=jax.ShapeDtypeStruct(conserved.shape, jnp.float32),
        in_specs=spec(VMEM, cores + 1),
        out_specs=pl.BlockSpec(memory_space=HBM),
        scratch_shapes=[pltpu.VMEM(conserved.shape, jnp.float32), pltpu.SemaphoreType.DMA((fields,))],
        compiler_params=limit(8),
        cost_estimate=work_for(10**6),
        name="inverse",
    )(modes, *others(modes), back)
    spectra = pl.pallas_call(
        functools.partial(spectra_kernel, sizes),
        out_shape=shape(1, share * CAP, NFREQ * 2 * NM),
        in_specs=spec(VMEM, peers) + spec(SMEM, 1),
        out_specs=pl.BlockSpec(memory_space=VMEM),
        compiler_params=limit(8),
        cost_estimate=work_for(10**6),
        name="spectra",
    )(*received, window_table)
    return (advanced, spectra)


def solution(mesh):
    in_specs = (
        P(None, "gx", "row", "ta"),
        P(),
        P(),
        P(),
        P(),
        P(("gx", "row")),
        P(("gx", "row"), None),
        P(),
    )
    out_specs = (P(None, "gx", "row", "ta"), P(("gx", "row"), "ta", None))

    def body(*args):
        return local(dict(mesh.shape), *args)

    return jax.shard_map(body, mesh=mesh, in_specs=in_specs, out_specs=out_specs, check_vma=False)
```
